128 devices in a mesh: rep: 1, r: 16 (over y, z), s: 8 (over x, core).
Axes of the slice: x: 4, y: 4, z: 4, core: 2. Of those that a mesh axis runs over, the one named last changes fastest.
Arguments:
- x: bfloat16 [128, 2048, 1024], P(('rep', 'r', 's'))
- dy: bfloat16 [128, 2048, 1024], P(('rep', 'r', 's'))
- w_gate: bfloat16 [2, 1024, 3584], P(None, 's')
- w_up: bfloat16 [2, 1024, 3584], P(None, 's')
- w_down: bfloat16 [2, 3584, 1024], P(None, 's')
- m_w_gate: float32 [2, 1024, 3584], P(None, 's')
- m_w_up: float32 [2, 1024, 3584], P(None, 's')
- m_w_down: float32 [2, 3584, 1024], P(None, 's')
- v_w_gate: float32 [2, 1024, 3584], P(None, 's')
- v_w_up: float32 [2, 1024, 3584], P(None, 's')
- v_w_down: float32 [2, 3584, 1024], P(None, 's')
Outputs:
- output 1: bfloat16 [2, 1024, 3584], P('rep', 's')
- output 2: bfloat16 [2, 1024, 3584], P('rep', 's')
- output 3: bfloat16 [2, 3584, 1024], P('rep', 's')
- output 4: float32 [2, 1024, 3584], P('rep', 's')
- output 5: float32 [2, 1024, 3584], P('rep', 's')
- output 6: float32 [2, 3584, 1024], P('rep', 's')
- output 7: float32 [2, 1024, 3584], P('rep', 's')
- output 8: float32 [2, 1024, 3584], P('rep', 's')
- output 9: float32 [2, 3584, 1024], P('rep', 's')
All inputs are finite; a program needn't handle non-finite values.
Results may differ from the reference program's by a relative error of at most 0.022.
Values are sent between devices in bfloat16 or wider.
A program may use at most 1.5 GiB of HBM per device.

```python
import jax
import jax.numpy as jnp
from jax import lax

SEQUENCES = 128
TOKENS = 2048
D = 1024
FF = 3584
LAYERS = 2
NAMES = ("w_gate", "w_up", "w_down")
SHAPES = {"w_gate": (LAYERS, D, FF), "w_up": (LAYERS, D, FF), "w_down": (LAYERS, FF, D)}


def bump(key, n, height):
    away = (jnp.arange(n, dtype=jnp.int32) - jax.random.randint(key, (), 0, n, jnp.int32)) % n
    return jnp.where(away < n // 8, height, 1.0)


def together(key, own, strength):
    shared = jax.random.normal(key, own.shape[1:], jnp.float32)
    return (own + strength * shared) * lax.rsqrt(1 + strength * strength)


def setup_inputs(seed: int = 0, part: int = 0) -> dict:
    kx, kdy, ka, kb, kz, kf, kh, kl, *keys = jax.random.split(jax.random.key(seed), 8 + 3 * len(NAMES))
    kx, kdy, ka, kb = (jax.random.fold_in(k, part) for k in (kx, kdy, ka, kb))
    kw, km, kv = (keys[i::3] for i in range(3))
    shape = (SEQUENCES, TOKENS, D)
    much_x, much_dy = jax.random.uniform(kz, (2,), jnp.float32, 0.0, 1.0)
    loud = 2.0 ** jax.random.uniform(jax.random.fold_in(kz, 1), (), jnp.float32, -1.0, 2.0)
    layers = 2.0 ** jax.random.uniform(kl, (LAYERS, 1, 1), jnp.float32, -1.0, 1.0)
    x = together(ka, jax.random.normal(kx, shape, jnp.float32), much_x) * bump(kf, D, 4.0)
    dy = together(kb, jax.random.normal(kdy, shape, jnp.float32), much_dy)
    drawn = {"x": x.astype(jnp.bfloat16), "dy": (loud * dy * (SEQUENCES * TOKENS) ** -0.5).astype(jnp.bfloat16)}
    for key, name in zip(kw, NAMES, strict=True):
        w = jax.random.normal(key, SHAPES[name], jnp.float32) * SHAPES[name][1] ** -0.5
        drawn[name] = (w * {"w_gate": 1.0, "w_up": bump(kh, FF, 4.0), "w_down": layers}[name]).astype(jnp.bfloat16)
    for key, name in zip(km, NAMES, strict=True):
        drawn[f"m_{name}"] = 0.1 * jax.random.normal(key, SHAPES[name], jnp.float32)
    for key, name in zip(kv, NAMES, strict=True):
        drawn[f"v_{name}"] = loud * loud * jax.random.uniform(key, SHAPES[name], jnp.float32, 0.05, 0.15)
    return drawn


def matmul(a, w):
    return jnp.dot(a, w, preferred_element_type=jnp.float32).astype(jnp.bfloat16)


def normed(h):
    wide = h.astype(jnp.float32)
    scale = lax.rsqrt(jnp.mean(wide**2, -1, keepdims=True) + 1e-6)
    return (wide * scale).astype(jnp.bfloat16)


def layer(h, w):
    a = normed(h)
    gate = jnp.dot(a, w["w_gate"], preferred_element_type=jnp.float32)
    up = jnp.dot(a, w["w_up"], preferred_element_type=jnp.float32)
    return h + matmul((jax.nn.silu(gate) * up).astype(jnp.bfloat16), w["w_down"])


def adamw(w, m, v, g):
    m = 0.9 * m + 0.1 * g
    v = 0.95 * v + 0.05 * g * g
    step = m * lax.rsqrt(v + 1e-8) + 0.1 * w
    return (w - 0.02 * step).astype(jnp.bfloat16), m, v


def stack(weights, h):
    return lax.scan(lambda h, w: (layer(h, w), None), h, weights)[0]


def reference(x, dy, w_gate, w_up, w_down, m_w_gate, m_w_up, m_w_down, v_w_gate, v_w_up, v_w_down):
    weights = dict(zip(NAMES, (w_gate, w_up, w_down), strict=True))

    def take(so_far, sequence):
        h, by_y = sequence
        _, back = jax.vjp(lambda w: stack(w, h), weights)
        return jax.tree.map(lambda total, term: total + term.astype(jnp.float32), so_far, back(by_y)[0]), None

    none_yet = {name: jnp.zeros(w.shape, jnp.float32) for name, w in weights.items()}
    by_weights, _ = lax.scan(take, none_yet, (x, dy))
    gradients = [by_weights[name].astype(jnp.bfloat16).astype(jnp.float32) for name in NAMES]
    new = [
        adamw(w.astype(jnp.float32), m, v, g)
        for w, m, v, g in zip((w_gate, w_up, w_down), (m_w_gate, m_w_up, m_w_down), (v_w_gate, v_w_up, v_w_down), gradients, strict=True)
    ]
    return tuple(one[which] for which in range(3) for one in new)
```

```python
import functools

import jax
import jax.numpy as jnp
from jax import lax
from jax.experimental import pallas as pl
from jax.experimental.pallas import tpu as pltpu
from jax.sharding import PartitionSpec as P

BF, F32 = jnp.bfloat16, jnp.float32
MIB = 1 << 20
TOKENS, D, FF = 2048, 1024, 3584
TN = 512
MESH = pl.DeviceIdType.MESH

NN = (((1,), (0,)), ((), ()))
NT = (((1,), (1,)), ((), ()))
TNN = (((0,), (0,)), ((), ()))


def dot(a, b, dims=NN):
    return lax.dot_general(a, b, dims, preferred_element_type=F32)


def params(**kw):
    return pltpu.CompilerParams(vmem_limit_bytes=60 * MIB, **kw)


def cost(flops, nbytes):
    return pl.CostEstimate(flops=flops, bytes_accessed=nbytes, transcendentals=0)


def normed(h):
    wide = h.astype(F32)
    scale = lax.rsqrt(jnp.mean(wide**2, -1, keepdims=True) + 1e-6)
    return (wide * scale).astype(BF)


def adamw(w, m, v, g):
    m = 0.9 * m + 0.1 * g
    v = 0.95 * v + 0.05 * g * g
    step = m * lax.rsqrt(v + 1e-8) + 0.1 * w
    return (w - 0.02 * step).astype(BF), m, v


def split_rows(rows, chunk):
    return [pl.ds(i * chunk, chunk) for i in range(rows // chunk)]


def gate_up_kernel(a_ref, wg_ref, wu_ref, hid_ref, gate_ref, up_ref):
    for rows in split_rows(a_ref.shape[0], 256):
        a = a_ref[rows, :]
        gate, up = dot(a, wg_ref[...]), dot(a, wu_ref[...])
        gate_ref[rows, :] = gate
        up_ref[rows, :] = up
        hid_ref[rows, :] = (gate * jax.nn.sigmoid(gate) * up).astype(BF)


def gate_up(a, w, first):
    tm, at = 1024, first * (FF // TN)
    tile = pl.BlockSpec((tm, TN), lambda j, i: (i, j))
    return pl.pallas_call(
        gate_up_kernel,
        grid=(FF // TN, TOKENS // tm),
        in_specs=[
            pl.BlockSpec((tm, D), lambda j, i: (i, 0)),
            pl.BlockSpec((D, TN), lambda j, i: (0, at + j)),
            pl.BlockSpec((D, TN), lambda j, i: (0, at + FF // TN + j)),
        ],
        out_specs=[tile, tile, tile],
        out_shape=[jax.ShapeDtypeStruct((TOKENS, FF), t) for t in (BF, F32, F32)],
        compiler_params=params(),
        cost_estimate=cost(4 * TOKENS * D * FF, 100 * MIB),
        name="gate_up",
    )(a, w, w)


def grads_of_act(gate, up, d_hidden):
    sig = jax.nn.sigmoid(gate)
    silu = gate * sig
    d = d_hidden.astype(BF).astype(F32)
    return silu * up, d * up * (sig + silu * (1.0 - sig)), d * silu


def last_layer_kernel(a_ref, dy_ref, wg_ref, wu_ref, wd_ref, hid_ref, dg_ref, du_ref):
    for rows in split_rows(a_ref.shape[0], 256):
        a = a_ref[rows, :]
        gate, up = dot(a, wg_ref[...]), dot(a, wu_ref[...])
        hid, dg, du = grads_of_act(gate, up, dot(dy_ref[rows, :], wd_ref[...], NT))
        hid_ref[rows, :] = hid.astype(BF)
        dg_ref[rows, :] = dg.astype(BF)
        du_ref[rows, :] = du.astype(BF)


def last_layer(a, dy, w, first, wd):
    tm, at = 1024, first * (FF // TN)
    tile = pl.BlockSpec((tm, TN), lambda j, i: (i, j))
    wide = pl.BlockSpec((tm, D), lambda j, i: (i, 0))
    return pl.pallas_call(
        last_layer_kernel,
        grid=(FF // TN, TOKENS // tm),
        in_specs=[
            wide,
            wide,
            pl.BlockSpec((D, TN), lambda j, i: (0, at + j)),
            pl.BlockSpec((D, TN), lambda j, i: (0, at + FF // TN + j)),
            pl.BlockSpec((TN, D), lambda j, i: (j, 0)),
        ],
        out_specs=[tile, tile, tile],
        out_shape=[jax.ShapeDtypeStruct((TOKENS, FF), BF)] * 3,
        compiler_params=params(),
        cost_estimate=cost(6 * TOKENS * D * FF, 80 * MIB),
        name="last_layer",
    )(a, dy, w, w, wd)


def act_grad_kernel(dh_ref, wd_ref, gate_ref, up_ref, dg_ref, du_ref):
    for rows in split_rows(dh_ref.shape[0], 256):
        _, dg, du = grads_of_act(gate_ref[rows, :], up_ref[rows, :], dot(dh_ref[rows, :], wd_ref[...], NT))
        dg_ref[rows, :] = dg.astype(BF)
        du_ref[rows, :] = du.astype(BF)


def act_grad(dh, wd, gate, up):
    tm = 1024
    tile = pl.BlockSpec((tm, TN), lambda j, i: (i, j))
    return pl.pallas_call(
        act_grad_kernel,
        grid=(FF // TN, TOKENS // tm),
        in_specs=[
            pl.BlockSpec((tm, D), lambda j, i: (i, 0)),
            pl.BlockSpec((TN, D), lambda j, i: (j, 0)),
            tile,
            tile,
        ],
        out_specs=[tile, tile],
        out_shape=[jax.ShapeDtypeStruct((TOKENS, FF), BF)] * 2,
        compiler_params=params(),
        cost_estimate=cost(2 * TOKENS * D * FF, 120 * MIB),
        name="act_grad",
    )(dh, wd, gate, up)


def norm_grad_kernel(dg_ref, du_ref, wg_ref, wu_ref, h_ref, dy_ref, dh_ref, acc):
    k = pl.program_id(1)
    both = dot(dg_ref[...], wg_ref[...], NT) + dot(du_ref[...], wu_ref[...], NT)

    @pl.when(k == 0)
    def _():
        acc[...] = both

    @pl.when(k > 0)
    def _():
        acc[...] += both

    @pl.when(k == pl.num_programs(1) - 1)
    def _():
        @pl.loop(0, acc.shape[0] // 128)
        def _(i):
            rows = pl.ds(pl.multiple_of(i * 128, 128), 128)
            da = acc[rows, :].astype(BF).astype(F32)
            wide = h_ref[rows, :].astype(F32)
            scale = lax.rsqrt(jnp.mean(wide * wide, -1, keepdims=True) + 1e-6)
            along = jnp.mean(da * wide, -1, keepdims=True)
            dh = (da * scale - wide * (scale * scale * scale * along)).astype(BF)
            dh_ref[rows, :] = dy_ref[rows, :] + dh


def norm_grad(dg, du, w, first, h, dy):
    tm, at = 1024, first * (FF // TN)
    tile = pl.BlockSpec((tm, TN), lambda i, k: (i, k))
    wide = pl.BlockSpec((tm, D), lambda i, k: (i, 0))
    return pl.pallas_call(
        norm_grad_kernel,
        grid=(TOKENS // tm, FF // TN),
        in_specs=[
            tile,
            tile,
            pl.BlockSpec((D, TN), lambda i, k: (0, at + k)),
            pl.BlockSpec((D, TN), lambda i, k: (0, at + FF // TN + k)),
            wide,
            wide,
        ],
        out_specs=wide,
        out_shape=jax.ShapeDtypeStruct((TOKENS, D), BF),
        scratch_shapes=[pltpu.VMEM((tm, D), F32)],
        compiler_params=params(),
        cost_estimate=cost(4 * TOKENS * D * FF, 60 * MIB),
        name="norm_grad",
    )(dg, du, w, w, h, dy)


class Place:
    def __init__(self):
        r, s = lax.axis_index("r"), lax.axis_index("s")
        self.r, self.s = r, s
        self.y, self.z = lax.div(r, 4), lax.rem(r, 4)
        self.x, self.c = lax.div(s, 2), lax.rem(s, 2)

    def partner(self):
        return (0, self.r, self.x * 2 + 1 - self.c)

    def along(self, axis, k):
        here = getattr(self, axis)
        there = lax.rem(here + k, 4)
        at = {"x": self.x, "y": self.y, "z": self.z, axis: there}
        return there, (0, at["y"] * 4 + at["z"], at["x"] * 2 + self.c)


def all_greet(me):
    barrier = pltpu.get_barrier_semaphore()
    peers = [me.partner()] + [me.along(axis, k)[1] for axis in "xyz" for k in (1, 2, 3)]
    for peer in peers:
        pl.semaphore_signal(barrier, inc=1, device_id=peer, device_id_type=MESH)
    pl.semaphore_wait(barrier, len(peers))


class Summed:
    def __init__(self, me, own, core, away, buffers, sems, out):
        self.me, self.own, self.core, self.away, self.out = me, own, core, away, out
        self.from_core, self.first, self.second, self.third = buffers
        self.send, self.recv, self.local = sems
        self.rows, self.cols = out.shape
        self.part, self.half = self.rows // 4, self.cols // 2
        self.flying = []

    def piece(self, color, where):
        rows = pl.ds(pl.multiple_of(where * self.part, self.part), self.part)
        return rows, pl.ds(color * self.half, self.half)

    def copy(self, stage, color, k, src, dst, device):
        one = pltpu.make_async_remote_copy(
            src_ref=src,
            dst_ref=dst,
            send_sem=self.send.at[stage, color, k],
            recv_sem=self.recv.at[stage, color, k],
            device_id=device,
            device_id_type=MESH,
        )
        return one

    def copies(self, stage):
        me = self.me
        if stage == 0:
            return [self.copy(0, 0, 0, self.away, self.from_core, me.partner())]
        made = []
        for color in (0, 1):
            main, other = ("y", "z") if color == 0 else ("z", "y")
            mine = getattr(me, main)
            for k in (1, 2, 3):
                if stage == 1:
                    there, device = me.along(main, k)
                    rows, cols = self.piece(color, there)
                    src, dst = self.own.at[:, self.core, rows, cols], self.first.at[color, k - 1]
                elif stage == 2:
                    there, device = me.along("x", k)
                    rows, cols = self.piece(color, mine)
                    src, dst = self.own.at[there, self.core, rows, cols], self.second.at[color, k - 1]
                elif stage == 3:
                    _, device = me.along(other, k)
                    rows, cols = self.piece(color, mine)
                    src, dst = self.own.at[me.x, self.core, rows, cols], self.third.at[color, getattr(me, other)]
                else:
                    _, device = me.along(main, k)
                    rows, cols = self.piece(color, mine)
                    src, dst = self.own.at[me.x, self.core, rows, cols], self.out.at[rows, cols]
                made.append(self.copy(stage, color, k - 1, src, dst, device))
        return made

    def locals_(self):
        made = []
        for color in (0, 1):
            rows, cols = self.piece(color, self.me.y if color == 0 else self.me.z)
            src = self.own.at[self.me.x, self.core, rows, cols]
            made.append(pltpu.make_async_copy(src, self.out.at[rows, cols], self.local.at[color]))
        return made

    def start(self, stage):
        me = self.me
        if stage == 3:
            for color in (0, 1):
                rows, cols = self.piece(color, me.y if color == 0 else me.z)
                self.third[color, me.z if color == 0 else me.y] = self.own[me.x, self.core, rows, cols]
        for one in self.copies(stage):
            one.start()
        if stage == 4:
            for one in self.locals_():
                one.start()

    def finish(self, stage):
        me, own, core = self.me, self.own, self.core
        for one in self.copies(stage):
            one.wait()
        if stage == 0:
            step = 32 if self.rows % 64 else 64
            step = 32 if self.cols > 1024 else step

            @pl.loop(0, 4)
            def _(x):
                @pl.loop(0, self.rows // step)
                def _(i):
                    rows = pl.ds(pl.multiple_of(i * step, step), step)
                    own[x, core, rows, :] = (own[x, core, rows, :].astype(F32) + self.from_core[x, rows, :].astype(F32)).astype(BF)

        elif stage == 1:
            for color in (0, 1):
                rows, cols = self.piece(color, me.y if color == 0 else me.z)

                @pl.loop(0, 4)
                def _(x, color=color, rows=rows, cols=cols):
                    total = own[x, core, rows, cols].astype(F32)
                    for k in range(3):
                        total += self.first[color, k, x].astype(F32)
                    own[x, core, rows, cols] = total.astype(BF)

        elif stage == 2:
            for color in (0, 1):
                rows, cols = self.piece(color, me.y if color == 0 else me.z)
                total = own[me.x, core, rows, cols].astype(F32)
                for k in range(3):
                    total += self.second[color, k].astype(F32)
                own[me.x, core, rows, cols] = total.astype(BF)
        elif stage == 3:
            for color in (0, 1):
                rows, cols = self.piece(color, me.y if color == 0 else me.z)
                total = self.third[color, 0].astype(F32)
                for k in range(1, 4):
                    total += self.third[color, k].astype(F32)
                own[me.x, core, rows, cols] = total.astype(BF)
        else:
            for one in self.locals_():
                one.wait()


def buffers_of(rows, cols):
    part, half = rows // 4, cols // 2
    return [
        pltpu.VMEM((4, rows, cols), BF),
        pltpu.VMEM((2, 3, 4, part, half), BF),
        pltpu.VMEM((2, 3, part, half), BF),
        pltpu.VMEM((2, 4, part, half), BF),
    ]


def sems_of():
    return [pltpu.SemaphoreType.DMA((5, 2, 3)), pltpu.SemaphoreType.DMA((5, 2, 3)), pltpu.SemaphoreType.DMA((2,))]


def first_layer_kernel(a_ref, dg_ref, du_ref, down_ref, gd_ref, gg_ref, gu_ref, own_d, term_g, term_u, load, *rest):
    i = pl.program_id(0)
    steps = FF // TN
    me = Place()
    parts = [(rest[7 * n : 7 * n + 4], rest[7 * n + 4 : 7 * n + 7]) for n in range(3)]
    down = Summed(me, own_d, 0, down_ref.at[:, 1 - me.c], *parts[0], gd_ref)
    gate = Summed(me, term_g, me.c, term_g.at[:, 1 - me.c], *parts[1], gg_ref)
    up = Summed(me, term_u, me.c, term_u.at[:, 1 - me.c], *parts[2], gu_ref)
    loading = pltpu.make_async_copy(down_ref.at[:, me.c], own_d.at[:, 0], load)

    @pl.when(i == 0)
    def _():
        all_greet(me)
        down.start(0)
        loading.start()

    for term, d_ref, first in ((term_g, dg_ref, 0), (term_u, du_ref, steps)):

        @pl.when(jnp.logical_and(i >= first, i < first + steps))
        def _(term=term, d_ref=d_ref, first=first):
            cols = pl.ds(pl.multiple_of((i - first) * TN, TN), TN)
            term[:, :, :, cols] = dot(a_ref[...], d_ref[...], TNN).astype(BF).reshape(4, 2, D // 8, TN)

    @pl.when(i == 2)
    def _():
        loading.wait()
        down.finish(0)
        down.start(1)

    @pl.when(i == steps - 1)
    def _():
        gate.start(0)

    @pl.when(i == steps + 2)
    def _():
        gate.finish(0)

    @pl.when(i == steps + 3)
    def _():
        down.finish(1)
        down.start(2)
        gate.start(1)

    @pl.when(i == 2 * steps - 1)
    def _():
        up.start(0)
        down.finish(2)
        down.start(3)
        up.finish(0)
        down.finish(3)
        down.start(4)
        up.start(1)
        gate.finish(1)
        gate.start(2)
        gate.finish(2)
        gate.start(3)
        gate.finish(3)
        gate.start(4)
        up.finish(1)
        up.start(2)
        up.finish(2)
        up.start(3)
        up.finish(3)
        up.start(4)
        for one in (down, gate, up):
            one.finish(4)


def first_layer_grads(a, dg, du, down):
    steps = FF // TN
    rows_d, rows = FF // 8, D // 8
    anywhere = pl.BlockSpec(memory_space=pl.ANY)
    gd, gg, gu = pl.pallas_call(
        first_layer_kernel,
        grid=(2 * steps,),
        in_specs=[
            pl.BlockSpec((TOKENS, D), lambda i: (0, 0), pipeline_mode=pl.Buffered(1)),
            pl.BlockSpec((TOKENS, TN), lambda i: (0, jnp.minimum(i, steps - 1))),
            pl.BlockSpec((TOKENS, TN), lambda i: (0, jnp.maximum(i - steps, 0))),
            anywhere,
        ],
        out_specs=[anywhere] * 3,
        out_shape=[
            jax.ShapeDtypeStruct((rows_d, D), BF),
            jax.ShapeDtypeStruct((rows, FF), BF),
            jax.ShapeDtypeStruct((rows, FF), BF),
        ],
        scratch_shapes=[
            pltpu.VMEM((4, 1, rows_d, D), BF),
            pltpu.VMEM((4, 2, rows, FF), BF),
            pltpu.VMEM((4, 2, rows, FF), BF),
            pltpu.SemaphoreType.DMA,
            *buffers_of(rows_d, D),
            *sems_of(),
            *buffers_of(rows, FF),
            *sems_of(),
            *buffers_of(rows, FF),
            *sems_of(),
        ],
        compiler_params=pltpu.CompilerParams(
            vmem_limit_bytes=67_043_328,
            collective_id=0,
            has_side_effects=True,
        ),
        cost_estimate=cost(4 * TOKENS * D * FF, 60 * MIB),
        name="first_layer_grads",
    )(a, dg, du, down.reshape(4, 2, rows_d, D))
    return gg, gu, gd


def solution(mesh):
    def step(x, dy, *arrays):
        weights, m, v = (arrays[i : i + 3] for i in (0, 3, 6))
        x, dy = x[0], dy[0]
        place = lax.axis_index("r")
        rows = weights[0].shape[1] // 16
        mine = [lax.dynamic_slice_in_dim(weights[n][layer], place * rows, rows, 0) for layer in (0, 1) for n in (0, 1)]
        w = lax.all_gather(jnp.concatenate(mine, 1), ("s", "r"), axis=0, tiled=True)
        wd = [lax.all_gather(weights[2][layer], "s", axis=0, tiled=True) for layer in (0, 1)]

        a0 = normed(x)
        hid0, gate0, up0 = gate_up(a0, w, 0)
        h1 = x + dot(hid0, wd[0]).astype(BF)
        a1 = normed(h1)
        hid1, dg1, du1 = last_layer(a1, dy, w, 2, wd[1])

        def scattered(term):
            return lax.psum_scatter(term, "s", scatter_dimension=0, tiled=True)

        terms = [scattered(dot(a, b, TNN).astype(BF)) for a, b in ((hid1, dy), (a1, dg1), (a1, du1))]
        dh1 = norm_grad(dg1, du1, w, 2, h1, dy)
        down0 = dot(hid0, dh1, TNN).astype(BF)
        dg0, du0 = act_grad(dh1, wd[0], gate0, up0)
        d1, g1, u1 = (lax.psum(t, "r") for t in terms)
        g0, u0, d0 = first_layer_grads(a0, dg0, du0, down0)
        gradients = [jnp.stack(pair).astype(F32) for pair in ((g0, g1), (u0, u1), (d0, d1))]
        new = [adamw(w.astype(F32), m, v, g) for w, m, v, g in zip(weights, m, v, gradients, strict=True)]
        return tuple(one[which] for which in range(3) for one in new)

    states, cut = P(("rep", "r", "s"), None, None), P(None, "s", None)
    return jax.shard_map(
        step,
        mesh=mesh,
        in_specs=(states, states) + (cut,) * 9,
        out_specs=(P("rep", "s", None),) * 9,
        check_vma=False,
    )
```

```python
import functools

import jax
import jax.numpy as jnp
from jax import lax
from jax.experimental import pallas as pl
from jax.experimental.pallas import tpu as pltpu
from jax.sharding import PartitionSpec as P

BF, F32 = jnp.bfloat16, jnp.float32
MIB = 1 << 20
TOKENS, D, FF = 2048, 1024, 3584
TN = 512
MESH = pl.DeviceIdType.MESH

NN = (((1,), (0,)), ((), ()))
NT = (((1,), (1,)), ((), ()))
TNN = (((0,), (0,)), ((), ()))


def dot(a, b, dims=NN):
    return lax.dot_general(a, b, dims, preferred_element_type=F32)


def params(**kw):
    return pltpu.CompilerParams(vmem_limit_bytes=60 * MIB, **kw)


def cost(flops, nbytes):
    return pl.CostEstimate(flops=flops, bytes_accessed=nbytes, transcendentals=0)


def normed(h):
    wide = h.astype(F32)
    scale = lax.rsqrt(jnp.mean(wide**2, -1, keepdims=True) + 1e-6)
    return (wide * scale).astype(BF)


def adamw(w, m, v, g):
    m = 0.9 * m + 0.1 * g
    v = 0.95 * v + 0.05 * g * g
    step = m * lax.rsqrt(v + 1e-8) + 0.1 * w
    return (w - 0.02 * step).astype(BF), m, v


def split_rows(rows, chunk):
    return [pl.ds(i * chunk, chunk) for i in range(rows // chunk)]


def grads_of_act(gate, up, d_hidden):
    sig = jax.nn.sigmoid(gate)
    silu = gate * sig
    d = d_hidden.astype(BF).astype(F32)
    return silu * up, d * up * (sig + silu * (1.0 - sig)), d * silu


def last_layer_kernel(a_ref, dy_ref, wg_ref, wu_ref, wd_ref, hid_ref, dg_ref, du_ref):
    for rows in split_rows(a_ref.shape[0], 256):
        a = a_ref[rows, :]
        gate, up = dot(a, wg_ref[...]), dot(a, wu_ref[...])
        hid, dg, du = grads_of_act(gate, up, dot(dy_ref[rows, :], wd_ref[...], NT))
        hid_ref[rows, :] = hid.astype(BF)
        dg_ref[rows, :] = dg.astype(BF)
        du_ref[rows, :] = du.astype(BF)


def last_layer(a, dy, w, wd):
    tn = 256
    tile = pl.BlockSpec((TOKENS, tn), lambda j: (0, j))
    wide = pl.BlockSpec((TOKENS, D), lambda j: (0, 0), pipeline_mode=pl.Buffered(1))
    return pl.pallas_call(
        last_layer_kernel,
        grid=(FF // tn,),
        in_specs=[
            wide,
            wide,
            pl.BlockSpec((D, tn), lambda j: (0, j)),
            pl.BlockSpec((D, tn), lambda j: (0, FF // tn + j)),
            pl.BlockSpec((tn, D), lambda j: (j, 0)),
        ],
        out_specs=[tile, tile, tile],
        out_shape=[jax.ShapeDtypeStruct((TOKENS, FF), BF)] * 3,
        compiler_params=params(),
        cost_estimate=cost(6 * TOKENS * D * FF, 80 * MIB),
        name="last_layer",
    )(a, dy, w, w, wd)


def act_grad_kernel(dh_ref, wd_ref, by_gate_ref, by_up_ref, dg_ref, du_ref):
    for rows in split_rows(dh_ref.shape[0], 256):
        d = dot(dh_ref[rows, :], wd_ref[...], NT).astype(BF).astype(F32)
        dg_ref[rows, :] = (d * by_gate_ref[rows, :]).astype(BF)
        du_ref[rows, :] = (d * by_up_ref[rows, :]).astype(BF)


def act_grad(dh, wd, by_gate, by_up):
    tile = pl.BlockSpec((TOKENS, TN), lambda j: (0, j))
    return pl.pallas_call(
        act_grad_kernel,
        grid=(FF // TN,),
        in_specs=[
            pl.BlockSpec((TOKENS, D), lambda j: (0, 0), pipeline_mode=pl.Buffered(1)),
            pl.BlockSpec((TN, D), lambda j: (j, 0)),
            tile,
            tile,
        ],
        out_specs=[tile, tile],
        out_shape=[jax.ShapeDtypeStruct((TOKENS, FF), BF)] * 2,
        compiler_params=params(),
        cost_estimate=cost(2 * TOKENS * D * FF, 120 * MIB),
        name="act_grad",
    )(dh, wd, by_gate, by_up)


def norm_grad_kernel(dg_ref, du_ref, wg_ref, wu_ref, h_ref, dy_ref, dh_ref, acc):
    k = pl.program_id(1)
    both = dot(dg_ref[...], wg_ref[...], NT) + dot(du_ref[...], wu_ref[...], NT)

    @pl.when(k == 0)
    def _():
        acc[...] = both

    @pl.when(k > 0)
    def _():
        acc[...] += both

    @pl.when(k == pl.num_programs(1) - 1)
    def _():
        @pl.loop(0, acc.shape[0] // 128)
        def _(i):
            rows = pl.ds(pl.multiple_of(i * 128, 128), 128)
            da = acc[rows, :].astype(BF).astype(F32)
            wide = h_ref[rows, :].astype(F32)
            scale = lax.rsqrt(jnp.mean(wide * wide, -1, keepdims=True) + 1e-6)
            along = jnp.mean(da * wide, -1, keepdims=True)
            dh = (da * scale - wide * (scale * scale * scale * along)).astype(BF)
            dh_ref[rows, :] = dy_ref[rows, :] + dh


def norm_grad(dg, du, w, h, dy):
    tm = 1024
    tile = pl.BlockSpec((tm, TN), lambda i, k: (i, k))
    wide = pl.BlockSpec((tm, D), lambda i, k: (i, 0))
    return pl.pallas_call(
        norm_grad_kernel,
        grid=(TOKENS // tm, FF // TN),
        in_specs=[
            tile,
            tile,
            pl.BlockSpec((D, TN), lambda i, k: (0, k)),
            pl.BlockSpec((D, TN), lambda i, k: (0, FF // TN + k)),
            wide,
            wide,
        ],
        out_specs=wide,
        out_shape=jax.ShapeDtypeStruct((TOKENS, D), BF),
        scratch_shapes=[pltpu.VMEM((tm, D), F32)],
        compiler_params=params(),
        cost_estimate=cost(4 * TOKENS * D * FF, 60 * MIB),
        name="norm_grad",
    )(dg, du, w, w, h, dy)


class Place:
    def __init__(self):
        r, s = lax.axis_index("r"), lax.axis_index("s")
        self.r, self.s = r, s
        self.y, self.z = lax.div(r, 4), lax.rem(r, 4)
        self.x, self.c = lax.div(s, 2), lax.rem(s, 2)

    def partner(self):
        return (0, self.r, self.x * 2 + 1 - self.c)

    def along(self, axis, k):
        here = getattr(self, axis)
        there = lax.rem(here + k, 4)
        at = {"x": self.x, "y": self.y, "z": self.z, axis: there}
        return there, (0, at["y"] * 4 + at["z"], at["x"] * 2 + self.c)


def all_greet(me):
    barrier = pltpu.get_barrier_semaphore()
    peers = [me.partner()] + [me.along(axis, k)[1] for axis in "xyz" for k in (1, 2, 3)]
    for peer in peers:
        pl.semaphore_signal(barrier, inc=1, device_id=peer, device_id_type=MESH)
    pl.semaphore_wait(barrier, len(peers))


GROUPS = ((0, 1), (1, 1), (2, 1), (3, 2), (5, 2))


class Gathered:
    def __init__(self, me, w, number, sems):
        self.me, self.number = me, number
        self.send, self.recv = sems
        first, count = GROUPS[number]
        self.w = w.at[pl.ds(first, count)]

    def rows(self, color):
        quarter = D // 64
        where = self.me.y if color == 0 else self.me.z
        return pl.ds(pl.multiple_of((color * 4 + where) * quarter, quarter), quarter)

    def copies(self, stage):
        me, w, made = self.me, self.w, []

        def copy(src, dst, color, k, device):
            at = (self.number, stage, color, k)
            made.append(pltpu.make_async_remote_copy(src_ref=src, dst_ref=dst, send_sem=self.send.at[at], recv_sem=self.recv.at[at], device_id=device, device_id_type=MESH))

        if stage == 2:
            copy(w.at[:, :, me.c], w.at[:, :, me.c], 0, 0, me.partner())
            return made
        for color in (0, 1):
            rows = self.rows(color)
            for k in (1, 2, 3):
                if stage == 0:
                    copy(w.at[:, 0, me.c, rows], w.at[:, 4 - k, me.c, rows], color, k - 1, me.along("x", k)[1])
                else:
                    others = w.at[:, pl.ds(1, 3), me.c, rows]
                    copy(others, others, color, k - 1, me.along("yz"[color], k)[1])
        return made

    def start(self, stage):
        for one in self.copies(stage):
            one.start()

    def finish(self, stage):
        for one in self.copies(stage):
            one.wait()


class GatheredDown:
    def __init__(self, me, own, out, held, sems):
        self.me, self.own, self.out, self.held = me, own, out, held
        self.send, self.recv, self.local = sems
        self.part, self.half = own.shape[0] // 4, own.shape[1] // 2

    def piece(self, color):
        where = self.me.y if color == 0 else self.me.z
        return pl.ds(pl.multiple_of(where * self.part, self.part), self.part), pl.ds(color * self.half, self.half)

    def copies(self, stage):
        me, out, made = self.me, self.out, []

        def copy(src, dst, n, device):
            at = (stage, n)
            made.append(pltpu.make_async_remote_copy(src_ref=src, dst_ref=dst, send_sem=self.send.at[at], recv_sem=self.recv.at[at], device_id=device, device_id_type=MESH))

        if stage == 2:
            copy(self.own, out.at[me.x, me.c], 0, me.partner())
            for k in (1, 2, 3):
                x, _ = me.along("x", k)
                copy(out.at[x, me.c], out.at[x, me.c], k, me.partner())
            return made
        for color in (0, 1):
            rows, cols = self.piece(color)
            for k in (1, 2, 3):
                if stage == 0:
                    copy(self.own.at[rows, cols], out.at[me.x, me.c, rows, cols], color * 3 + k - 1, me.along("x", k)[1])
                    continue
                for other in (1, 2, 3):
                    there = out.at[me.along("x", other)[0], me.c, rows, cols]
                    copy(there, there, (color * 3 + k - 1) * 3 + other - 1, me.along("yz"[color], k)[1])
        return made

    def taken(self):
        return pltpu.make_async_copy(self.own, self.held, self.local.at[0])

    def put(self):
        return pltpu.make_async_copy(self.held, self.out.at[self.me.x, self.me.c], self.local.at[1])

    def start(self, stage):
        for one in self.copies(stage):
            one.start()

    def finish(self, stage):
        for one in self.copies(stage):
            one.wait()


def first_layer_forward_kernel(x_ref, wg_ref, wu_ref, wd_ref, hid_ref, by_gate_ref, by_up_ref, wd0_ref, wd1_ref, w, a, held0, held1, load, *sems):
    j = pl.program_id(0)
    me = Place()
    groups = [Gathered(me, w, n, sems[:2]) for n in range(len(GROUPS))]
    downs = [GatheredDown(me, wd_ref.at[n], out, held, sems[2 + 3 * n : 5 + 3 * n]) for n, (out, held) in enumerate(((wd0_ref, held0), (wd1_ref, held1)))]
    loads = []
    for chunk in range(FF // TN):
        for n, ref in enumerate((wg_ref, wu_ref)):
            src = ref.at[0, :, pl.ds(chunk * TN, TN)]
            loads.append(pltpu.make_async_copy(src, w.at[chunk, 0, me.c, :, pl.ds(n * TN, TN)], load.at[chunk, n]))

    def onward(which, stage):
        which.finish(stage)
        which.start(stage + 1)

    @pl.when(j == 0)
    def _():
        for one in loads:
            one.start()
        for down in downs:
            down.taken().start()
        all_greet(me)
        for one in loads:
            one.wait()
        for group in groups:
            group.start(0)

        @pl.loop(0, TOKENS // 128)
        def _(i):
            rows = pl.ds(pl.multiple_of(i * 128, 128), 128)
            wide = x_ref[rows, :].astype(F32)
            scale = lax.rsqrt(jnp.mean(wide**2, -1, keepdims=True) + 1e-6)
            for k in range(4):
                there, _ = me.along("x", k)
                cols = pl.ds(pl.multiple_of(there * (D // 4), D // 4), D // 4)
                a[rows, pl.ds(k * (D // 4), D // 4)] = (x_ref[rows, cols].astype(F32) * scale).astype(BF)

        onward(groups[0], 0)
        onward(groups[1], 0)
        onward(groups[0], 1)
        onward(groups[2], 0)
        groups[0].finish(2)
        for down in downs:
            down.taken().wait()
            down.put().start()

    def part(rows_of):
        for rows in rows_of:
            both = dot(a[rows, :], w[j].reshape(D, 2 * TN))
            gate, up = both[:, :TN], both[:, TN:]
            sig = jax.nn.sigmoid(gate)
            silu = gate * sig
            by_up_ref[rows, :] = silu
            by_gate_ref[rows, :] = up * (sig + silu * (1.0 - sig))
            hid_ref[rows, :] = (silu * up).astype(BF)

    rows_of = split_rows(TOKENS, 256)
    part(rows_of[:4])

    @pl.when(j == 0)
    def _():
        onward(groups[1], 1)
        onward(groups[3], 0)
        downs[0].start(0)

    @pl.when(j == 1)
    def _():
        onward(groups[2], 1)
        onward(groups[4], 0)
        downs[1].start(0)

    @pl.when(j == 2)
    def _():
        onward(groups[3], 1)

    @pl.when(j == 4)
    def _():
        onward(groups[4], 1)
        onward(downs[1], 0)

    part(rows_of[4:])

    @pl.when(j == 0)
    def _():
        groups[1].finish(2)

    @pl.when(j == 1)
    def _():
        groups[2].finish(2)

    @pl.when(j == 2)
    def _():
        groups[3].finish(2)

    @pl.when(j == 3)
    def _():
        onward(downs[0], 0)

    @pl.when(j == 4)
    def _():
        groups[4].finish(2)

    @pl.when(j == 6)
    def _():
        for down in downs:
            onward(down, 1)
        for down in downs:
            down.finish(2)
            down.put().wait()


def first_layer_forward(x, wg, wu, wd):
    tile = pl.BlockSpec((TOKENS, TN), lambda j: (0, j))
    anywhere = pl.BlockSpec(memory_space=pl.ANY)
    full = jax.ShapeDtypeStruct((4, 2, FF // 8, D), BF)
    dma = pltpu.SemaphoreType.DMA
    hid, by_gate, by_up, wd0, wd1 = pl.pallas_call(
        first_layer_forward_kernel,
        grid=(FF // TN,),
        in_specs=[pl.BlockSpec((TOKENS, D), lambda j: (0, 0), pipeline_mode=pl.Buffered(1)), anywhere, anywhere, anywhere],
        out_specs=[tile, tile, tile, anywhere, anywhere],
        out_shape=[jax.ShapeDtypeStruct((TOKENS, FF), t) for t in (BF, F32, F32)] + [full, full],
        scratch_shapes=[
            pltpu.VMEM((FF // TN, 4, 2, D // 8, 2 * TN), BF),
            pltpu.VMEM((TOKENS, D), BF),
            pltpu.VMEM((FF // 8, D), BF),
            pltpu.VMEM((FF // 8, D), BF),
            dma((FF // TN, 2)),
            dma((len(GROUPS), 3, 2, 3)),
            dma((len(GROUPS), 3, 2, 3)),
            *[dma((3, 18)), dma((3, 18)), dma((2,))] * 2,
        ],
        compiler_params=pltpu.CompilerParams(vmem_limit_bytes=60 * MIB, collective_id=1, has_side_effects=True),
        cost_estimate=cost(4 * TOKENS * D * FF, 100 * MIB),
        name="first_layer_forward",
    )(x, wg, wu, wd)
    return hid, by_gate, by_up, wd0.reshape(FF, D), wd1.reshape(FF, D)


class Summed:
    def __init__(self, me, own, core, away, buffers, sems, out):
        self.me, self.own, self.core, self.away, self.out = me, own, core, away, out
        self.from_core, self.first, self.second, self.third = buffers
        self.send, self.recv, self.local = sems
        self.rows, self.cols = out.shape
        self.part, self.half = self.rows // 4, self.cols // 2
        self.flying = []

    def piece(self, color, where):
        rows = pl.ds(pl.multiple_of(where * self.part, self.part), self.part)
        return rows, pl.ds(color * self.half, self.half)

    def copy(self, stage, color, k, src, dst, device):
        one = pltpu.make_async_remote_copy(
            src_ref=src,
            dst_ref=dst,
            send_sem=self.send.at[stage, color, k],
            recv_sem=self.recv.at[stage, color, k],
            device_id=device,
            device_id_type=MESH,
        )
        return one

    def copies(self, stage):
        me = self.me
        if stage == 0:
            return [self.copy(0, 0, 0, self.away, self.from_core, me.partner())]
        made = []
        for color in (0, 1):
            main, other = ("y", "z") if color == 0 else ("z", "y")
            mine = getattr(me, main)
            for k in (1, 2, 3):
                if stage == 1:
                    there, device = me.along(main, k)
                    rows, cols = self.piece(color, there)
                    src, dst = self.own.at[:, self.core, rows, cols], self.first.at[color, k - 1]
                elif stage == 2:
                    there, device = me.along("x", k)
                    rows, cols = self.piece(color, mine)
                    src, dst = self.own.at[there, self.core, rows, cols], self.second.at[color, k - 1]
                elif stage == 3:
                    _, device = me.along(other, k)
                    rows, cols = self.piece(color, mine)
                    src, dst = self.own.at[me.x, self.core, rows, cols], self.third.at[color, getattr(me, other)]
                else:
                    _, device = me.along(main, k)
                    rows, cols = self.piece(color, mine)
                    src, dst = self.own.at[me.x, self.core, rows, cols], self.out.at[rows, cols]
                made.append(self.copy(stage, color, k - 1, src, dst, device))
        return made

    def locals_(self):
        made = []
        for color in (0, 1):
            rows, cols = self.piece(color, self.me.y if color == 0 else self.me.z)
            src = self.own.at[self.me.x, self.core, rows, cols]
            made.append(pltpu.make_async_copy(src, self.out.at[rows, cols], self.local.at[color]))
        return made

    def start(self, stage):
        me = self.me
        if stage == 3:
            for color in (0, 1):
                rows, cols = self.piece(color, me.y if color == 0 else me.z)
                self.third[color, me.z if color == 0 else me.y] = self.own[me.x, self.core, rows, cols]
        for one in self.copies(stage):
            one.start()
        if stage == 4:
            for one in self.locals_():
                one.start()

    def finish(self, stage):
        me, own, core = self.me, self.own, self.core
        for one in self.copies(stage):
            one.wait()
        if stage == 0:
            step = 32 if self.rows % 64 else 64
            step = 32 if self.cols > 1024 else step

            @pl.loop(0, 4)
            def _(x):
                @pl.loop(0, self.rows // step)
                def _(i):
                    rows = pl.ds(pl.multiple_of(i * step, step), step)
                    own[x, core, rows, :] = (own[x, core, rows, :].astype(F32) + self.from_core[x, rows, :].astype(F32)).astype(BF)

        elif stage == 1:
            for color in (0, 1):
                rows, cols = self.piece(color, me.y if color == 0 else me.z)

                @pl.loop(0, 4)
                def _(x, color=color, rows=rows, cols=cols):
                    total = own[x, core, rows, cols].astype(F32)
                    for k in range(3):
                        total += self.first[color, k, x].astype(F32)
                    own[x, core, rows, cols] = total.astype(BF)

        elif stage == 2:
            for color in (0, 1):
                rows, cols = self.piece(color, me.y if color == 0 else me.z)
                total = own[me.x, core, rows, cols].astype(F32)
                for k in range(3):
                    total += self.second[color, k].astype(F32)
                own[me.x, core, rows, cols] = total.astype(BF)
        elif stage == 3:
            for color in (0, 1):
                rows, cols = self.piece(color, me.y if color == 0 else me.z)
                total = self.third[color, 0].astype(F32)
                for k in range(1, 4):
                    total += self.third[color, k].astype(F32)
                own[me.x, core, rows, cols] = total.astype(BF)
        else:
            for one in self.locals_():
                one.wait()


def buffers_of(rows, cols):
    part, half = rows // 4, cols // 2
    return [
        pltpu.VMEM((4, rows, cols), BF),
        pltpu.VMEM((2, 3, 4, part, half), BF),
        pltpu.VMEM((2, 3, part, half), BF),
        pltpu.VMEM((2, 4, part, half), BF),
    ]


def sems_of():
    return [pltpu.SemaphoreType.DMA((5, 2, 3)), pltpu.SemaphoreType.DMA((5, 2, 3)), pltpu.SemaphoreType.DMA((2,))]


def first_layer_kernel(a_ref, dg_ref, du_ref, down_ref, gd_ref, gg_ref, gu_ref, own_d, term_g, term_u, load, *rest):
    i = pl.program_id(0)
    steps = FF // TN
    me = Place()
    parts = [(rest[7 * n : 7 * n + 4], rest[7 * n + 4 : 7 * n + 7]) for n in range(3)]
    down = Summed(me, own_d, 0, down_ref.at[:, 1 - me.c], *parts[0], gd_ref)
    gate = Summed(me, term_g, me.c, term_g.at[:, 1 - me.c], *parts[1], gg_ref)
    up = Summed(me, term_u, me.c, term_u.at[:, 1 - me.c], *parts[2], gu_ref)
    loading = pltpu.make_async_copy(down_ref.at[:, me.c], own_d.at[:, 0], load)

    @pl.when(i == 0)
    def _():
        all_greet(me)
        down.start(0)
        loading.start()

    for term, d_ref, first in ((term_g, dg_ref, 0), (term_u, du_ref, steps)):

        @pl.when(jnp.logical_and(i >= first, i < first + steps))
        def _(term=term, d_ref=d_ref, first=first):
            cols = pl.ds(pl.multiple_of((i - first) * TN, TN), TN)
            term[:, :, :, cols] = dot(a_ref[...], d_ref[...], TNN).astype(BF).reshape(4, 2, D // 8, TN)

    @pl.when(i == 2)
    def _():
        loading.wait()
        down.finish(0)
        down.start(1)

    @pl.when(i == steps - 1)
    def _():
        gate.start(0)

    @pl.when(i == steps + 2)
    def _():
        gate.finish(0)

    @pl.when(i == steps + 3)
    def _():
        down.finish(1)
        down.start(2)
        gate.start(1)

    @pl.when(i == 2 * steps - 1)
    def _():
        up.start(0)
        down.finish(2)
        down.start(3)
        up.finish(0)
        down.finish(3)
        down.start(4)
        up.start(1)
        gate.finish(1)
        gate.start(2)
        gate.finish(2)
        gate.start(3)
        gate.finish(3)
        gate.start(4)
        up.finish(1)
        up.start(2)
        up.finish(2)
        up.start(3)
        up.finish(3)
        up.start(4)
        for one in (down, gate, up):
            one.finish(4)


def first_layer_grads(a, dg, du, down):
    steps = FF // TN
    rows_d, rows = FF // 8, D // 8
    anywhere = pl.BlockSpec(memory_space=pl.ANY)
    gd, gg, gu = pl.pallas_call(
        first_layer_kernel,
        grid=(2 * steps,),
        in_specs=[
            pl.BlockSpec((TOKENS, D), lambda i: (0, 0), pipeline_mode=pl.Buffered(1)),
            pl.BlockSpec((TOKENS, TN), lambda i: (0, jnp.minimum(i, steps - 1))),
            pl.BlockSpec((TOKENS, TN), lambda i: (0, jnp.maximum(i - steps, 0))),
            anywhere,
        ],
        out_specs=[anywhere] * 3,
        out_shape=[
            jax.ShapeDtypeStruct((rows_d, D), BF),
            jax.ShapeDtypeStruct((rows, FF), BF),
            jax.ShapeDtypeStruct((rows, FF), BF),
        ],
        scratch_shapes=[
            pltpu.VMEM((4, 1, rows_d, D), BF),
            pltpu.VMEM((4, 2, rows, FF), BF),
            pltpu.VMEM((4, 2, rows, FF), BF),
            pltpu.SemaphoreType.DMA,
            *buffers_of(rows_d, D),
            *sems_of(),
            *buffers_of(rows, FF),
            *sems_of(),
            *buffers_of(rows, FF),
            *sems_of(),
        ],
        compiler_params=pltpu.CompilerParams(
            vmem_limit_bytes=67_043_328,
            collective_id=0,
            has_side_effects=True,
        ),
        cost_estimate=cost(4 * TOKENS * D * FF, 60 * MIB),
        name="first_layer_grads",
    )(a, dg, du, down.reshape(4, 2, rows_d, D))
    return gg, gu, gd


def solution(mesh):
    def step(x, dy, *arrays):
        weights, m, v = (arrays[i : i + 3] for i in (0, 3, 6))
        x, dy = x[0], dy[0]
        place, rows = lax.axis_index("r"), weights[0].shape[1] // 16
        mine = [lax.dynamic_slice(w, (1, place * rows, 0), (1, rows, FF))[0] for w in weights[:2]]
        w1 = lax.all_gather(jnp.concatenate(mine, 1), ("s", "r"), axis=0, tiled=True)

        hid0, by_gate0, by_up0, wd0, wd1 = first_layer_forward(x, *weights)
        h1 = x + dot(hid0, wd0).astype(BF)
        a1 = normed(h1)
        hid1, dg1, du1 = last_layer(a1, dy, w1, wd1)

        def scattered(term):
            return lax.psum_scatter(term, "s", scatter_dimension=0, tiled=True)

        terms = [scattered(dot(a, b, TNN).astype(BF)) for a, b in ((hid1, dy), (a1, dg1), (a1, du1))]
        dh1 = norm_grad(dg1, du1, w1, h1, dy)
        down0 = dot(hid0, dh1, TNN).astype(BF)
        dg0, du0 = act_grad(dh1, wd0, by_gate0, by_up0)
        a0 = normed(x)
        d1, g1, u1 = (lax.psum(t, "r") for t in terms)
        g0, u0, d0 = first_layer_grads(a0, dg0, du0, down0)
        gradients = [jnp.stack(pair).astype(F32) for pair in ((g0, g1), (u0, u1), (d0, d1))]
        new = [adamw(w.astype(F32), m, v, g) for w, m, v, g in zip(weights, m, v, gradients, strict=True)]
        return tuple(one[which] for which in range(3) for one in new)

    states, cut = P(("rep", "r", "s"), None, None), P(None, "s", None)
    return jax.shard_map(
        step,
        mesh=mesh,
        in_specs=(states, states) + (cut,) * 9,
        out_specs=(P("rep", "s", None),) * 9,
        check_vma=False,
    )
```

```python
import jax
import jax.numpy as jnp
from jax import lax
from jax.experimental import pallas as pl
from jax.experimental.pallas import tpu as pltpu
from jax.sharding import PartitionSpec as P

BF, F32 = jnp.bfloat16, jnp.float32
MIB = 1 << 20
TOKENS, D, FF = 2048, 1024, 3584
TN = 512
MESH = pl.DeviceIdType.MESH

NN = (((1,), (0,)), ((), ()))
NT = (((1,), (1,)), ((), ()))
TNN = (((0,), (0,)), ((), ()))


def dot(a, b, dims=NN):
    return lax.dot_general(a, b, dims, preferred_element_type=F32)


def params(**kw):
    return pltpu.CompilerParams(vmem_limit_bytes=60 * MIB, **kw)


def cost(flops, nbytes):
    return pl.CostEstimate(flops=flops, bytes_accessed=nbytes, transcendentals=0)


def normed(h):
    wide = h.astype(F32)
    scale = lax.rsqrt(jnp.mean(wide**2, -1, keepdims=True) + 1e-6)
    return (wide * scale).astype(BF)


def adamw(w, m, v, g):
    m = 0.9 * m + 0.1 * g
    v = 0.95 * v + 0.05 * g * g
    step = m * lax.rsqrt(v + 1e-8) + 0.1 * w
    return (w - 0.02 * step).astype(BF), m, v


def split_rows(rows, chunk):
    return [pl.ds(i * chunk, chunk) for i in range(rows // chunk)]


def grads_of_act(gate, up, d_hidden):
    sig = jax.nn.sigmoid(gate)
    silu = gate * sig
    d = d_hidden.astype(BF).astype(F32)
    return silu * up, d * up * (sig + silu * (1.0 - sig)), d * silu


def last_layer_kernel(a_ref, dy_ref, wg_ref, wu_ref, wd_ref, hid_ref, dg_ref, du_ref):
    for rows in split_rows(a_ref.shape[0], 256):
        a = a_ref[rows, :]
        gate, up = dot(a, wg_ref[...]), dot(a, wu_ref[...])
        hid, dg, du = grads_of_act(gate, up, dot(dy_ref[rows, :], wd_ref[...], NT))
        hid_ref[rows, :] = hid.astype(BF)
        dg_ref[rows, :] = dg.astype(BF)
        du_ref[rows, :] = du.astype(BF)


def last_layer(a, dy, w, wd):
    tn = 256
    tile = pl.BlockSpec((TOKENS, tn), lambda j: (0, j))
    wide = pl.BlockSpec((TOKENS, D), lambda j: (0, 0), pipeline_mode=pl.Buffered(1))
    return pl.pallas_call(
        last_layer_kernel,
        grid=(FF // tn,),
        in_specs=[
            wide,
            wide,
            pl.BlockSpec((D, tn), lambda j: (0, j)),
            pl.BlockSpec((D, tn), lambda j: (0, FF // tn + j)),
            pl.BlockSpec((tn, D), lambda j: (j, 0)),
        ],
        out_specs=[tile, tile, tile],
        out_shape=[jax.ShapeDtypeStruct((TOKENS, FF), BF)] * 3,
        compiler_params=params(),
        cost_estimate=cost(6 * TOKENS * D * FF, 80 * MIB),
        name="last_layer",
    )(a, dy, w, w, wd)


class Place:
    def __init__(self):
        r, s = lax.axis_index("r"), lax.axis_index("s")
        self.r, self.s = r, s
        self.y, self.z = lax.div(r, 4), lax.rem(r, 4)
        self.x, self.c = lax.div(s, 2), lax.rem(s, 2)

    def partner(self):
        return (0, self.r, self.x * 2 + 1 - self.c)

    def along(self, axis, k):
        here = getattr(self, axis)
        there = lax.rem(here + k, 4)
        at = {"x": self.x, "y": self.y, "z": self.z, axis: there}
        return there, (0, at["y"] * 4 + at["z"], at["x"] * 2 + self.c)


def all_greet(me):
    barrier = pltpu.get_barrier_semaphore()
    peers = [me.partner()] + [me.along(axis, k)[1] for axis in "xyz" for k in (1, 2, 3)]
    for peer in peers:
        pl.semaphore_signal(barrier, inc=1, device_id=peer, device_id_type=MESH)
    pl.semaphore_wait(barrier, len(peers))


GROUPS = ((0, 1), (1, 1), (2, 1), (3, 2), (5, 2))


class Gathered:
    def __init__(self, me, w, number, sems):
        self.me, self.number, self.stage = me, number, -1
        self.send, self.recv = sems
        first, count = GROUPS[number]
        self.w = w.at[pl.ds(first, count)]

    def rows(self, color):
        quarter = D // 64
        where = self.me.y if color == 0 else self.me.z
        return pl.ds(pl.multiple_of((color * 4 + where) * quarter, quarter), quarter)

    def copies(self, stage):
        me, w, made = self.me, self.w, []

        def copy(src, dst, color, k, device):
            at = (self.number, stage, color, k)
            made.append(pltpu.make_async_remote_copy(src_ref=src, dst_ref=dst, send_sem=self.send.at[at], recv_sem=self.recv.at[at], device_id=device, device_id_type=MESH))

        if stage == 2:
            copy(w.at[:, :, me.c], w.at[:, :, me.c], 0, 0, me.partner())
            return made
        for color in (0, 1):
            rows = self.rows(color)
            for k in (1, 2, 3):
                if stage == 0:
                    copy(w.at[:, 0, me.c, rows], w.at[:, 4 - k, me.c, rows], color, k - 1, me.along("x", k)[1])
                else:
                    others = w.at[:, pl.ds(1, 3), me.c, rows]
                    copy(others, others, color, k - 1, me.along("yz"[color], k)[1])
        return made

    def advance(self):
        if self.stage >= 0:
            for one in self.copies(self.stage):
                one.wait()
        self.stage += 1
        if self.stage < 3:
            for one in self.copies(self.stage):
                one.start()


class GatheredDown:
    def __init__(self, me, own, out, held, sems):
        self.me, self.own, self.out, self.held, self.stage = me, own, out, held, -1
        self.send, self.recv, self.local = sems
        self.part, self.half = own.shape[0] // 4, own.shape[1] // 2

    def piece(self, color):
        where = self.me.y if color == 0 else self.me.z
        return pl.ds(pl.multiple_of(where * self.part, self.part), self.part), pl.ds(color * self.half, self.half)

    def copies(self, stage):
        me, out, made = self.me, self.out, []

        def copy(src, dst, n, device):
            at = (stage, n)
            made.append(pltpu.make_async_remote_copy(src_ref=src, dst_ref=dst, send_sem=self.send.at[at], recv_sem=self.recv.at[at], device_id=device, device_id_type=MESH))

        if stage == 2:
            copy(self.own, out.at[me.x, me.c], 0, me.partner())
            for k in (1, 2, 3):
                x, _ = me.along("x", k)
                copy(out.at[x, me.c], out.at[x, me.c], k, me.partner())
            return made
        for color in (0, 1):
            rows, cols = self.piece(color)
            for k in (1, 2, 3):
                if stage == 0:
                    copy(self.own.at[rows, cols], out.at[me.x, me.c, rows, cols], color * 3 + k - 1, me.along("x", k)[1])
                    continue
                for other in (1, 2, 3):
                    there = out.at[me.along("x", other)[0], me.c, rows, cols]
                    copy(there, there, (color * 3 + k - 1) * 3 + other - 1, me.along("yz"[color], k)[1])
        return made

    def taken(self):
        return pltpu.make_async_copy(self.own, self.held, self.local.at[0])

    def put(self):
        return pltpu.make_async_copy(self.held, self.out.at[self.me.x, self.me.c], self.local.at[1])

    def advance(self):
        if self.stage >= 0:
            for one in self.copies(self.stage):
                one.wait()
        self.stage += 1
        if self.stage < 3:
            for one in self.copies(self.stage):
                one.start()


FORWARD_STEPS = (("bdm", "b"), ("cen", "c"), ("d", "d"), ("", "m"), ("en", "e"), ("", ""), ("", "mnmn"))
FORWARD_MIDWAY, FORWARD_AFTER = zip(*FORWARD_STEPS, strict=True)


def first_layer_forward_kernel(x_ref, wg_ref, wu_ref, wd_ref, hid_ref, by_gate_ref, by_up_ref, wd0_ref, wd1_ref, a0_ref, w, a, held0, held1, load, out, *sems):
    j = pl.program_id(0)
    me = Place()
    groups = [Gathered(me, w, n, sems[:2]) for n in range(len(GROUPS))]
    downs = [GatheredDown(me, wd_ref.at[n], out, held, sems[2 + 3 * n : 5 + 3 * n]) for n, (out, held) in enumerate(((wd0_ref, held0), (wd1_ref, held1)))]
    named = dict(zip("abcdemn", groups + downs, strict=True))
    loads = []
    for chunk in range(FF // TN):
        for n, ref in enumerate((wg_ref, wu_ref)):
            src = ref.at[0, :, pl.ds(chunk * TN, TN)]
            loads.append(pltpu.make_async_copy(src, w.at[chunk, 0, me.c, :, pl.ds(n * TN, TN)], load.at[chunk, n]))

    saves = []
    for k in range(4):
        cols = pl.ds(pl.multiple_of(me.along("x", k)[0] * (D // 4), D // 4), D // 4)
        saves.append(pltpu.make_async_copy(a.at[:, pl.ds(k * (D // 4), D // 4)], a0_ref.at[:, cols], out.at[k]))

    @pl.when(j == 0)
    def _():
        for one in loads:
            one.start()
        for down in downs:
            down.taken().start()
        all_greet(me)
        for one in loads:
            one.wait()
        for group in groups:
            group.advance()

        @pl.loop(0, TOKENS // 128)
        def _(i):
            rows = pl.ds(pl.multiple_of(i * 128, 128), 128)
            wide = x_ref[rows, :].astype(F32)
            scale = lax.rsqrt(jnp.mean(wide**2, -1, keepdims=True) + 1e-6)
            for k in range(4):
                there, _ = me.along("x", k)
                cols = pl.ds(pl.multiple_of(there * (D // 4), D // 4), D // 4)
                a[rows, pl.ds(k * (D // 4), D // 4)] = (x_ref[rows, cols].astype(F32) * scale).astype(BF)

        for name in "abaca":
            named[name].advance()
        for down in downs:
            down.taken().wait()
            down.put().start()
        for one in saves:
            one.start()

    def part(rows_of):
        for rows in rows_of:
            both = dot(a[rows, :], w[j].reshape(D, 2 * TN))
            gate, up = both[:, :TN], both[:, TN:]
            sig = jax.nn.sigmoid(gate)
            silu = gate * sig
            by_up_ref[rows, :] = silu
            by_gate_ref[rows, :] = up * (sig + silu * (1.0 - sig))
            hid_ref[rows, :] = (silu * up).astype(BF)

    rows_of = split_rows(TOKENS, 256)
    part(rows_of[: len(rows_of) // 2])
    run_schedule(j, FORWARD_MIDWAY, named)
    part(rows_of[len(rows_of) // 2 :])
    run_schedule(j, FORWARD_AFTER, named)

    @pl.when(j == pl.num_programs(0) - 1)
    def _():
        for one in saves + [down.put() for down in downs]:
            one.wait()


def first_layer_forward(x, wg, wu, wd):
    tile = pl.BlockSpec((TOKENS, TN), lambda j: (0, j))
    anywhere = pl.BlockSpec(memory_space=pl.ANY)
    full = jax.ShapeDtypeStruct((4, 2, FF // 8, D), BF)
    dma = pltpu.SemaphoreType.DMA
    hid, by_gate, by_up, wd0, wd1, a0 = pl.pallas_call(
        first_layer_forward_kernel,
        grid=(FF // TN,),
        in_specs=[pl.BlockSpec((TOKENS, D), lambda j: (0, 0), pipeline_mode=pl.Buffered(1)), anywhere, anywhere, anywhere],
        out_specs=[tile, tile, tile, anywhere, anywhere, anywhere],
        out_shape=[jax.ShapeDtypeStruct((TOKENS, FF), t) for t in (BF, F32, F32)] + [full, full, jax.ShapeDtypeStruct((TOKENS, D), BF)],
        scratch_shapes=[
            pltpu.VMEM((FF // TN, 4, 2, D // 8, 2 * TN), BF),
            pltpu.VMEM((TOKENS, D), BF),
            pltpu.VMEM((FF // 8, D), BF),
            pltpu.VMEM((FF // 8, D), BF),
            dma((FF // TN, 2)),
            dma((4,)),
            dma((len(GROUPS), 3, 2, 3)),
            dma((len(GROUPS), 3, 2, 3)),
            *[dma((3, 18)), dma((3, 18)), dma((2,))] * 2,
        ],
        compiler_params=pltpu.CompilerParams(vmem_limit_bytes=60 * MIB, collective_id=1, has_side_effects=True),
        cost_estimate=cost(4 * TOKENS * D * FF, 100 * MIB),
        name="first_layer_forward",
    )(x, wg, wu, wd)
    return hid, by_gate, by_up, wd0.reshape(FF, D), wd1.reshape(FF, D), a0


SUM_GROUPS = ((0, 2), (2, 2), (4, 2), (6, 1))
STAGES = 5


class Summed:
    def __init__(self, me, term, core, away, buffers, sems, at, place):
        self.me, self.term, self.core, self.away, self.place, self.at = me, term, core, away, place, at
        self.from_core, self.first, self.second, self.third = buffers
        self.send, self.recv, self.local = sems
        self.count, self.part = term.shape[0], term.shape[-2] // 4
        self.stage = -1

    def rows(self, where):
        return pl.ds(pl.multiple_of(where * self.part, self.part), self.part)

    def axes(self, color):
        main, other = ("y", "z") if color == 0 else ("z", "y")
        return main, other, self.rows(getattr(self.me, main))

    def copies(self, stage):
        me, term, core, made = self.me, self.term, self.core, []

        def copy(src, dst, color, k, device):
            at = (*self.at, stage, color, k)
            made.append(pltpu.make_async_remote_copy(src_ref=src, dst_ref=dst, send_sem=self.send.at[at], recv_sem=self.recv.at[at], device_id=device, device_id_type=MESH))

        if stage == 0:
            for n, (src, dst) in enumerate(self.away):
                copy(src, dst, n, 0, me.partner())
            return made
        for color in range(2):
            main, other, mine = self.axes(color)
            for k in range(3):
                there, device = me.along({2: "x", 3: other}.get(stage, main), k + 1)
                if stage == 1:
                    copy(term.at[:, color, :, core, self.rows(there)], self.first.at[:, color, k], color, k, device)
                elif stage == 2:
                    copy(term.at[:, color, there, core, mine], self.second.at[:, color, k], color, k, device)
                elif stage == 3:
                    copy(term.at[:, color, me.x, core, mine], self.third.at[:, color, getattr(me, other)], color, k, device)
                else:
                    for n, (src, dst) in enumerate(self.outward(color)):
                        copy(src, dst, color, 3 * n + k, device)
        return made

    def outward(self, color):
        rows = self.axes(color)[-1]
        return [(self.term.at[n, color, self.me.x, self.core, rows], self.place(n, color, rows)) for n in range(self.count)]

    def kept(self):
        return [pltpu.make_async_copy(src, dst, self.local.at[(*self.at, color, n)]) for color in range(2) for n, (src, dst) in enumerate(self.outward(color))]

    def advance(self):
        assert self.stage < STAGES
        if self.stage >= 0:
            self.finish(self.stage)
        self.stage += 1
        if self.stage < STAGES:
            self.start(self.stage)

    def start(self, stage):
        me = self.me
        if stage == 3:
            for color in range(2):
                _, other, rows = self.axes(color)
                self.third[:, color, getattr(me, other)] = self.term[:, color, me.x, self.core, rows]
        for one in self.copies(stage):
            one.start()
        if stage == 4:
            for one in self.kept():
                one.start()

    def finish(self, stage):
        me, term, core = self.me, self.term, self.core
        for one in self.copies(stage):
            one.wait()
        if stage == 4:
            for one in self.kept():
                one.wait()
            return

        @pl.loop(0, self.count)
        def _(n):
            for color in range(2):
                mine = self.axes(color)[-1]
                if stage <= 1:

                    @pl.loop(0, 4)
                    def _(x, color=color, mine=mine):
                        if stage == 0:

                            @pl.loop(0, 4)
                            def _(quarter):
                                rows = self.rows(quarter)
                                total = term[n, color, x, core, rows].astype(F32) + self.from_core[n, color, x, rows].astype(F32)
                                term[n, color, x, core, rows] = total.astype(BF)

                        else:
                            total = term[n, color, x, core, mine].astype(F32)
                            for k in range(3):
                                total += self.first[n, color, k, x].astype(F32)
                            term[n, color, x, core, mine] = total.astype(BF)

                    continue
                if stage == 2:
                    total = term[n, color, me.x, core, mine].astype(F32)
                    parts = [self.second[n, color, k] for k in range(3)]
                else:
                    total, *parts = [self.third[n, color, k].astype(F32) for k in range(4)]
                for one in parts:
                    total += one.astype(F32)
                term[n, color, me.x, core, mine] = total.astype(BF)


def sum_buffers(tiles, rows, cols, from_core=None):
    part = rows // 4
    return [
        pltpu.VMEM((*(from_core or (tiles,)), 2, 4, rows, cols), BF),
        pltpu.VMEM((tiles, 2, 3, 4, part, cols), BF),
        pltpu.VMEM((tiles, 2, 3, part, cols), BF),
        pltpu.VMEM((tiles, 2, 4, part, cols), BF),
    ]


def sum_sems(*groups):
    dma = pltpu.SemaphoreType.DMA
    return [dma((*groups, STAGES, 2, 6)), dma((*groups, STAGES, 2, 6)), dma((*groups, 2, 2))]


class SummedDown:
    def __init__(self, me, term, own, buffers, sems, load, out):
        half = out.shape[-1] // 2
        cols = [pl.ds(n * half, half) for n in range(2)]
        away = [(term.at[:, 1 - me.c, :, c], buffers[0].at[0, n]) for n, c in enumerate(cols)]
        self.loads = [pltpu.make_async_copy(term.at[:, me.c, :, c], own.at[0, n, :, 0], load.at[n]) for n, c in enumerate(cols)]
        self.sum = Summed(me, own, 0, away, buffers, sems, (), lambda n, color, rows: out.at[rows, cols[color]])

    def advance(self):
        if self.sum.stage < 0:
            for one in self.loads:
                one.start()
        elif self.sum.stage == 0:
            for one in self.loads:
                one.wait()
        self.sum.advance()


def down_scratch():
    rows, half = FF // 8, D // 2
    own = pltpu.VMEM((1, 2, 4, 1, rows, half), BF)
    return [own, *sum_buffers(1, rows, half), *sum_sems(), pltpu.SemaphoreType.DMA((2,))]


def summed_down(me, term, out, scratch):
    return SummedDown(me, term, scratch[0], scratch[1:5], scratch[5:8], scratch[8], out)


def run_schedule(i, schedule, named):
    for at, names in enumerate(schedule):

        @pl.when(i == at)
        def _(names=names):
            for name in names:
                named[name].advance()


GRADS_SCHEDULE = ("", "d", "", "a", "a", "", "d", "b", "ba", "d", "a", "cdb", "ca", "ebcebceceebdace")


def first_layer_kernel(a_ref, dh_ref, wd_ref, by_gate_ref, by_up_ref, down_ref, gd_ref, gg_ref, gu_ref, term, both, *rest):
    i = pl.program_id(0)
    me = Place()
    scratch = len(down_scratch())
    named = {"d": summed_down(me, down_ref, gd_ref, rest[:scratch])}
    from_core, *others = rest[scratch : scratch + 4]
    for number, (first, count) in enumerate(SUM_GROUPS):
        tiles = pl.ds(first, count)
        mine, received = term.at[tiles], from_core.at[number % 2, pl.ds(0, count)]

        def place(n, color, rows, first=first):
            return (gg_ref, gu_ref)[color].at[rows, pl.ds((first + n) * TN, TN)]

        away = [(mine.at[:, :, :, 1 - me.c], received)]
        named["abce"[number]] = Summed(me, mine, me.c, away, [received, *(one.at[tiles] for one in others)], rest[scratch + 4 :], (number,), place)

    @pl.when(i == 0)
    def _():
        all_greet(me)
        named["d"].advance()

    half = TN // 2
    for rows in split_rows(TOKENS, 256):
        d = dot(dh_ref[rows, :], wd_ref[...], NT).astype(BF).astype(F32)
        both[rows, :half] = (d * by_gate_ref[rows, :]).astype(BF)
        both[rows, half:] = (d * by_up_ref[rows, :]).astype(BF)
    made = dot(a_ref[...], both[...], TNN).astype(BF)
    cols = pl.ds(pl.multiple_of(lax.rem(i, 2) * half, half), half)
    for n in range(2):
        term[lax.div(i, 2), n, :, :, :, cols] = made[:, n * half : (n + 1) * half].reshape(4, 2, D // 8, half)

    run_schedule(i, GRADS_SCHEDULE, named)


def first_layer_grads(a, dh, wd, by_gate, by_up, down):
    rows_d, rows, tiles, half = FF // 8, D // 8, FF // TN, TN // 2
    anywhere = pl.BlockSpec(memory_space=pl.ANY)
    wide = pl.BlockSpec((TOKENS, D), lambda i: (0, 0), pipeline_mode=pl.Buffered(1))
    tile = pl.BlockSpec((TOKENS, half), lambda i: (0, i))
    gd, gg, gu = pl.pallas_call(
        first_layer_kernel,
        grid=(2 * tiles,),
        in_specs=[wide, wide, pl.BlockSpec((half, D), lambda i: (i, 0)), tile, tile, anywhere],
        out_specs=[anywhere] * 3,
        out_shape=[jax.ShapeDtypeStruct(shape, BF) for shape in ((rows_d, D), (rows, FF), (rows, FF))],
        scratch_shapes=[
            pltpu.VMEM((tiles, 2, 4, 2, rows, TN), BF),
            pltpu.VMEM((TOKENS, TN), BF),
            *down_scratch(),
            *sum_buffers(tiles, rows, TN, (2, 2)),
            *sum_sems(len(SUM_GROUPS)),
        ],
        compiler_params=pltpu.CompilerParams(vmem_limit_bytes=67_043_328, collective_id=0, has_side_effects=True),
        cost_estimate=cost(6 * TOKENS * D * FF, 80 * MIB),
        name="first_layer_grads",
    )(a, dh, wd, by_gate, by_up, down)
    return gg, gu, gd


NORM_SCHEDULE = ("", "", "d", "", "", "", "", "", "", "d", "", "", "", "d", "", "", "d", "", "", "", "d")


def norm_grad_kernel(dg_ref, du_ref, wg_ref, wu_ref, h_ref, dy_ref, hid_ref, down1_ref, dh_ref, down_ref, gd_ref, acc, *rest):
    i, steps, tm = pl.program_id(0), FF // TN, acc.shape[0]
    me = Place()
    named = {"d": summed_down(me, down1_ref, gd_ref, rest)}

    @pl.when(i == 0)
    def _():
        all_greet(me)
        named["d"].advance()

    for part in range(2):
        first = part * steps

        @pl.when(jnp.logical_and(i >= first, i < first + steps))
        def _(part=part, first=first):
            both = dot(dg_ref[...], wg_ref[...], NT) + dot(du_ref[...], wu_ref[...], NT)
            acc[...] = jnp.where(i == first, both, acc[...] + both)

        @pl.when(i == first + steps - 1)
        def _(part=part):
            @pl.loop(0, tm // 128)
            def _(n):
                rows = pl.ds(pl.multiple_of(n * 128, 128), 128)
                da = acc[rows, :].astype(BF).astype(F32)
                wide = h_ref[rows, :].astype(F32)
                scale = lax.rsqrt(jnp.mean(wide * wide, -1, keepdims=True) + 1e-6)
                along = jnp.mean(da * wide, -1, keepdims=True)
                dh = (da * scale - wide * (scale * scale * scale * along)).astype(BF)
                dh_ref[pl.ds(pl.multiple_of(part * tm + n * 128, 128), 128), :] = dy_ref[rows, :] + dh

    @pl.when(i >= 2 * steps)
    def _():
        down_ref[...] = dot(hid_ref[...], dh_ref[...], TNN).astype(BF)

    run_schedule(i, NORM_SCHEDULE, named)


def norm_grad(dg, du, w, h, dy, hid, down1):
    tm, steps = TOKENS // 2, FF // TN

    def k(i):
        return jnp.where(i < 2 * steps, lax.rem(i, steps), steps - 1)

    def m(i):
        return jnp.minimum(lax.div(i, steps), 1)

    def last(i):
        return jnp.maximum(i - 2 * steps, 0)

    anywhere = pl.BlockSpec(memory_space=pl.ANY)
    tile = pl.BlockSpec((tm, TN), lambda i: (m(i), k(i)))
    wide = pl.BlockSpec((tm, D), lambda i: (m(i), 0))
    return pl.pallas_call(
        norm_grad_kernel,
        grid=(3 * steps,),
        in_specs=[
            tile,
            tile,
            pl.BlockSpec((D, TN), lambda i: (0, k(i))),
            pl.BlockSpec((D, TN), lambda i: (0, steps + k(i))),
            wide,
            wide,
            pl.BlockSpec((TOKENS, TN), lambda i: (0, last(i))),
            anywhere,
        ],
        out_specs=[pl.BlockSpec((TOKENS, D), lambda i: (0, 0)), pl.BlockSpec((TN, D), lambda i: (last(i), 0)), anywhere],
        out_shape=[jax.ShapeDtypeStruct(shape, BF) for shape in ((TOKENS, D), (FF, D), (FF // 8, D))],
        scratch_shapes=[pltpu.VMEM((tm, D), F32), *down_scratch()],
        compiler_params=params(collective_id=2, has_side_effects=True),
        cost_estimate=cost(6 * TOKENS * D * FF, 60 * MIB),
        name="norm_grad",
    )(dg, du, w, w, h, dy, hid, down1)


def solution(mesh):
    def step(x, dy, *arrays):
        weights, m, v = (arrays[i : i + 3] for i in (0, 3, 6))
        x, dy = x[0], dy[0]
        place, rows = lax.axis_index("r"), weights[0].shape[1] // 16
        mine = [lax.dynamic_slice(w, (1, place * rows, 0), (1, rows, FF))[0] for w in weights[:2]]
        w1 = lax.all_gather(jnp.concatenate(mine, 1), ("s", "r"), axis=0, tiled=True)

        hid0, by_gate0, by_up0, wd0, wd1, a0 = first_layer_forward(x, *weights)
        h1 = x + dot(hid0, wd0).astype(BF)
        a1 = normed(h1)
        hid1, dg1, du1 = last_layer(a1, dy, w1, wd1)

        def scattered(term):
            return lax.psum_scatter(term, "s", scatter_dimension=0, tiled=True)

        terms = [dot(a1, d, TNN).astype(BF) for d in (dg1, du1)]
        hid1, *_ = lax.optimization_barrier((hid1, *terms))
        terms = [scattered(one) for one in terms]
        down1 = dot(hid1, dy, TNN).astype(BF)
        by_core = (4, 2, FF // 8, D)
        dh1, down0, d1 = norm_grad(dg1, du1, w1, h1, dy, hid0, down1.reshape(by_core))
        *terms, dh1 = lax.optimization_barrier((*terms, dh1))
        g1, u1 = (lax.psum(t, "r") for t in terms)
        g0, u0, d0 = first_layer_grads(a0, dh1, wd0, by_gate0, by_up0, down0.reshape(by_core))
        gradients = [jnp.stack(pair).astype(F32) for pair in ((g0, g1), (u0, u1), (d0, d1))]
        new = [adamw(w.astype(F32), m, v, g) for w, m, v, g in zip(weights, m, v, gradients, strict=True)]
        return tuple(one[which] for which in range(3) for one in new)

    states, cut = P(("rep", "r", "s"), None, None), P(None, "s", None)
    return jax.shard_map(
        step,
        mesh=mesh,
        in_specs=(states, states) + (cut,) * 9,
        out_specs=(P("rep", "s", None),) * 9,
        check_vma=False,
    )
```

```python
import jax
import jax.numpy as jnp
from jax import lax
from jax.experimental import pallas as pl
from jax.experimental.pallas import tpu as pltpu
from jax.sharding import PartitionSpec as P

BF, F32 = jnp.bfloat16, jnp.float32
MIB = 1 << 20
TOKENS, D, FF = 2048, 1024, 3584
TN = 512
MESH = pl.DeviceIdType.MESH

NN = (((1,), (0,)), ((), ()))
NT = (((1,), (1,)), ((), ()))
TNN = (((0,), (0,)), ((), ()))


def dot(a, b, dims=NN):
    return lax.dot_general(a, b, dims, preferred_element_type=F32)


def params(**kw):
    return pltpu.CompilerParams(vmem_limit_bytes=60 * MIB, **kw)


def cost(flops, nbytes):
    return pl.CostEstimate(flops=flops, bytes_accessed=nbytes, transcendentals=0)


def normed(h):
    wide = h.astype(F32)
    scale = lax.rsqrt(jnp.mean(wide**2, -1, keepdims=True) + 1e-6)
    return (wide * scale).astype(BF)


def adamw(w, m, v, g):
    m = 0.9 * m + 0.1 * g
    v = 0.95 * v + 0.05 * g * g
    step = m * lax.rsqrt(v + 1e-8) + 0.1 * w
    return (w - 0.02 * step).astype(BF), m, v


def split_rows(rows, chunk):
    return [pl.ds(i * chunk, chunk) for i in range(rows // chunk)]


def grads_of_act(gate, up, d_hidden):
    sig = jax.nn.sigmoid(gate)
    silu = gate * sig
    d = d_hidden.astype(BF).astype(F32)
    return silu * up, d * up * (sig + silu * (1.0 - sig)), d * silu


def last_layer_kernel(a_ref, dy_ref, wg_ref, wu_ref, wd_ref, hid_ref, dg_ref, du_ref):
    for rows in split_rows(a_ref.shape[0], 256):
        a = a_ref[rows, :]
        gate, up = dot(a, wg_ref[...]), dot(a, wu_ref[...])
        hid, dg, du = grads_of_act(gate, up, dot(dy_ref[rows, :], wd_ref[...], NT))
        hid_ref[rows, :] = hid.astype(BF)
        dg_ref[rows, :] = dg.astype(BF)
        du_ref[rows, :] = du.astype(BF)


def last_layer(a, dy, w, wd):
    tn = 256
    tile = pl.BlockSpec((TOKENS, tn), lambda j: (0, j))
    wide = pl.BlockSpec((TOKENS, D), lambda j: (0, 0), pipeline_mode=pl.Buffered(1))
    return pl.pallas_call(
        last_layer_kernel,
        grid=(FF // tn,),
        in_specs=[
            wide,
            wide,
            pl.BlockSpec((D, tn), lambda j: (0, j)),
            pl.BlockSpec((D, tn), lambda j: (0, FF // tn + j)),
            pl.BlockSpec((tn, D), lambda j: (j, 0)),
        ],
        out_specs=[tile, tile, tile],
        out_shape=[jax.ShapeDtypeStruct((TOKENS, FF), BF)] * 3,
        compiler_params=params(),
        cost_estimate=cost(6 * TOKENS * D * FF, 80 * MIB),
        name="last_layer",
    )(a, dy, w, w, wd)


def down_kernel(hid_ref, wd_ref, x_ref, h_ref, a_ref):
    h = x_ref[...] + dot(hid_ref[...], wd_ref[...]).astype(BF)
    h_ref[...] = h
    a_ref[...] = normed(h)


def down(hid, wd, x):
    tm = 256
    wide = pl.BlockSpec((tm, D), lambda i: (i, 0))
    return pl.pallas_call(
        down_kernel,
        grid=(TOKENS // tm,),
        in_specs=[pl.BlockSpec((tm, FF), lambda i: (i, 0)), pl.BlockSpec((FF, D), lambda i: (0, 0), pipeline_mode=pl.Buffered(1)), wide],
        out_specs=[wide, wide],
        out_shape=[jax.ShapeDtypeStruct((TOKENS, D), BF)] * 2,
        compiler_params=params(),
        cost_estimate=cost(2 * TOKENS * D * FF, 40 * MIB),
        name="down",
    )(hid, wd, x)


def weight_grad_kernel(a_ref, b_ref, out_ref):
    out_ref[...] = dot(a_ref[...], b_ref[...], TNN).astype(BF)


def weight_grad(a, b):
    rows, cols = a.shape[-1], b.shape[-1]
    whole = pl.Buffered(1)
    left = pl.BlockSpec((TOKENS, rows), lambda i: (0, 0), pipeline_mode=whole) if rows < cols else pl.BlockSpec((TOKENS, TN), lambda i: (0, i))
    right = pl.BlockSpec((TOKENS, TN), lambda i: (0, i)) if rows < cols else pl.BlockSpec((TOKENS, cols), lambda i: (0, 0), pipeline_mode=whole)
    out = pl.BlockSpec((rows, TN), lambda i: (0, i)) if rows < cols else pl.BlockSpec((TN, cols), lambda i: (i, 0))
    return pl.pallas_call(
        weight_grad_kernel,
        grid=(FF // TN,),
        in_specs=[left, right],
        out_specs=out,
        out_shape=jax.ShapeDtypeStruct((rows, cols), BF),
        compiler_params=params(),
        cost_estimate=cost(2 * TOKENS * D * FF, 30 * MIB),
        name="weight_grad",
    )(a, b)


class Place:
    def __init__(self):
        r, s = lax.axis_index("r"), lax.axis_index("s")
        self.r, self.s = r, s
        self.y, self.z = lax.div(r, 4), lax.rem(r, 4)
        self.x, self.c = lax.div(s, 2), lax.rem(s, 2)

    def partner(self):
        return (0, self.r, self.x * 2 + 1 - self.c)

    def along(self, axis, k):
        here = getattr(self, axis)
        there = lax.rem(here + k, 4)
        at = {"x": self.x, "y": self.y, "z": self.z, axis: there}
        return there, (0, at["y"] * 4 + at["z"], at["x"] * 2 + self.c)


def all_greet(me):
    barrier = pltpu.get_barrier_semaphore()
    peers = [me.partner()] + [me.along(axis, k)[1] for axis in "xyz" for k in (1, 2, 3)]
    for peer in peers:
        pl.semaphore_signal(barrier, inc=1, device_id=peer, device_id_type=MESH)
    pl.semaphore_wait(barrier, len(peers))


GROUPS = ((0, 1), (1, 1), (2, 1), (3, 2), (5, 2))


class Gathered:
    def __init__(self, me, w, number, sems):
        self.me, self.number, self.stage = me, number, -1
        self.send, self.recv = sems
        first, count = GROUPS[number]
        self.w = w.at[pl.ds(first, count)]

    def rows(self, color):
        quarter = D // 64
        where = self.me.y if color == 0 else self.me.z
        return pl.ds(pl.multiple_of((color * 4 + where) * quarter, quarter), quarter)

    def copies(self, stage):
        me, w, made = self.me, self.w, []

        def copy(src, dst, color, k, device):
            at = (self.number, stage, color, k)
            made.append(pltpu.make_async_remote_copy(src_ref=src, dst_ref=dst, send_sem=self.send.at[at], recv_sem=self.recv.at[at], device_id=device, device_id_type=MESH))

        if stage == 2:
            copy(w.at[:, :, me.c], w.at[:, :, me.c], 0, 0, me.partner())
            return made
        for color in (0, 1):
            rows = self.rows(color)
            for k in (1, 2, 3):
                if stage == 0:
                    copy(w.at[:, 0, me.c, rows], w.at[:, 4 - k, me.c, rows], color, k - 1, me.along("x", k)[1])
                else:
                    others = w.at[:, pl.ds(1, 3), me.c, rows]
                    copy(others, others, color, k - 1, me.along("yz"[color], k)[1])
        return made

    def advance(self):
        if self.stage >= 0:
            for one in self.copies(self.stage):
                one.wait()
        self.stage += 1
        if self.stage < 3:
            for one in self.copies(self.stage):
                one.start()


class GatheredDown:
    def __init__(self, me, own, out, held, sems):
        self.me, self.own, self.out, self.held, self.stage = me, own, out, held, -1
        self.send, self.recv, self.local = sems
        self.part, self.half = own.shape[0] // 4, own.shape[1] // 2

    def piece(self, color):
        where = self.me.y if color == 0 else self.me.z
        return pl.ds(pl.multiple_of(where * self.part, self.part), self.part), pl.ds(color * self.half, self.half)

    def copies(self, stage):
        me, out, made = self.me, self.out, []

        def copy(src, dst, n, device):
            at = (stage, n)
            made.append(pltpu.make_async_remote_copy(src_ref=src, dst_ref=dst, send_sem=self.send.at[at], recv_sem=self.recv.at[at], device_id=device, device_id_type=MESH))

        if stage == 2:
            copy(self.own, out.at[me.x, me.c], 0, me.partner())
            for k in (1, 2, 3):
                x, _ = me.along("x", k)
                copy(out.at[x, me.c], out.at[x, me.c], k, me.partner())
            return made
        for color in (0, 1):
            rows, cols = self.piece(color)
            for k in (1, 2, 3):
                if stage == 0:
                    copy(self.own.at[rows, cols], out.at[me.x, me.c, rows, cols], color * 3 + k - 1, me.along("x", k)[1])
                    continue
                for other in (1, 2, 3):
                    there = out.at[me.along("x", other)[0], me.c, rows, cols]
                    copy(there, there, (color * 3 + k - 1) * 3 + other - 1, me.along("yz"[color], k)[1])
        return made

    def taken(self):
        return pltpu.make_async_copy(self.own, self.held, self.local.at[0])

    def put(self):
        return pltpu.make_async_copy(self.held, self.out.at[self.me.x, self.me.c], self.local.at[1])

    def advance(self):
        if self.stage >= 0:
            for one in self.copies(self.stage):
                one.wait()
        self.stage += 1
        if self.stage < 3:
            for one in self.copies(self.stage):
                one.start()


FORWARD_STEPS = (("bd", "b"), ("ce", "c"), ("dm", "dn"), ("", ""), ("e", "e"), ("", ""), ("", "mnmn"))
FORWARD_MIDWAY, FORWARD_AFTER = zip(*FORWARD_STEPS, strict=True)


def first_layer_forward_kernel(x_ref, wg_ref, wu_ref, wd_ref, hid_ref, by_gate_ref, by_up_ref, wd0_ref, wd1_ref, a0_ref, w, a, held0, held1, load, out, *sems):
    j = pl.program_id(0)
    me = Place()
    groups = [Gathered(me, w, n, sems[:2]) for n in range(len(GROUPS))]
    downs = [GatheredDown(me, wd_ref.at[n], out, held, sems[2 + 3 * n : 5 + 3 * n]) for n, (out, held) in enumerate(((wd0_ref, held0), (wd1_ref, held1)))]
    named = dict(zip("abcdemn", groups + downs, strict=True))
    loads = []
    for chunk in range(FF // TN):
        for n, ref in enumerate((wg_ref, wu_ref)):
            src = ref.at[0, :, pl.ds(chunk * TN, TN)]
            loads.append(pltpu.make_async_copy(src, w.at[chunk, 0, me.c, :, pl.ds(n * TN, TN)], load.at[chunk, n]))

    saves = []
    for k in range(4):
        cols = pl.ds(pl.multiple_of(me.along("x", k)[0] * (D // 4), D // 4), D // 4)
        saves.append(pltpu.make_async_copy(a.at[:, pl.ds(k * (D // 4), D // 4)], a0_ref.at[:, cols], out.at[k]))

    @pl.when(j == 0)
    def _():
        for one in loads:
            one.start()
        for down in downs:
            down.taken().start()
        all_greet(me)
        for one in loads:
            one.wait()
        for group in groups:
            group.advance()

        @pl.loop(0, TOKENS // 128)
        def _(i):
            rows = pl.ds(pl.multiple_of(i * 128, 128), 128)
            wide = x_ref[rows, :].astype(F32)
            scale = lax.rsqrt(jnp.mean(wide**2, -1, keepdims=True) + 1e-6)
            for k in range(4):
                there, _ = me.along("x", k)
                cols = pl.ds(pl.multiple_of(there * (D // 4), D // 4), D // 4)
                a[rows, pl.ds(k * (D // 4), D // 4)] = (x_ref[rows, cols].astype(F32) * scale).astype(BF)

        for name in "abacamn":
            named[name].advance()
        for down in downs:
            down.taken().wait()
            down.put().start()
        for one in saves:
            one.start()

    def part(rows_of):
        for rows in rows_of:
            both = dot(a[rows, :], w[j].reshape(D, 2 * TN))
            gate, up = both[:, :TN], both[:, TN:]
            sig = jax.nn.sigmoid(gate)
            silu = gate * sig
            by_up_ref[rows, :] = silu
            by_gate_ref[rows, :] = up * (sig + silu * (1.0 - sig))
            hid_ref[rows, :] = (silu * up).astype(BF)

    rows_of = split_rows(TOKENS, 256)
    part(rows_of[: len(rows_of) // 2])
    run_schedule(j, FORWARD_MIDWAY, named)
    part(rows_of[len(rows_of) // 2 :])
    run_schedule(j, FORWARD_AFTER, named)

    @pl.when(j == pl.num_programs(0) - 1)
    def _():
        for one in saves + [down.put() for down in downs]:
            one.wait()


def first_layer_forward(x, wg, wu, wd):
    tile = pl.BlockSpec((TOKENS, TN), lambda j: (0, j))
    anywhere = pl.BlockSpec(memory_space=pl.ANY)
    full = jax.ShapeDtypeStruct((4, 2, FF // 8, D), BF)
    dma = pltpu.SemaphoreType.DMA
    hid, by_gate, by_up, wd0, wd1, a0 = pl.pallas_call(
        first_layer_forward_kernel,
        grid=(FF // TN,),
        in_specs=[pl.BlockSpec((TOKENS, D), lambda j: (0, 0), pipeline_mode=pl.Buffered(1)), anywhere, anywhere, anywhere],
        out_specs=[tile, tile, tile, anywhere, anywhere, anywhere],
        out_shape=[jax.ShapeDtypeStruct((TOKENS, FF), t) for t in (BF, F32, F32)] + [full, full, jax.ShapeDtypeStruct((TOKENS, D), BF)],
        scratch_shapes=[
            pltpu.VMEM((FF // TN, 4, 2, D // 8, 2 * TN), BF),
            pltpu.VMEM((TOKENS, D), BF),
            pltpu.VMEM((FF // 8, D), BF),
            pltpu.VMEM((FF // 8, D), BF),
            dma((FF // TN, 2)),
            dma((4,)),
            dma((len(GROUPS), 3, 2, 3)),
            dma((len(GROUPS), 3, 2, 3)),
            *[dma((3, 18)), dma((3, 18)), dma((2,))] * 2,
        ],
        compiler_params=pltpu.CompilerParams(vmem_limit_bytes=60 * MIB, collective_id=1, has_side_effects=True),
        cost_estimate=cost(4 * TOKENS * D * FF, 100 * MIB),
        name="first_layer_forward",
    )(x, wg, wu, wd)
    return hid, by_gate, by_up, wd0.reshape(FF, D), wd1.reshape(FF, D), a0


SUM_GROUPS = ((0, 2), (2, 2), (4, 2), (6, 1))
STAGES = 5


class Summed:
    def __init__(self, me, term, core, away, buffers, sems, at, place):
        self.me, self.term, self.core, self.away, self.place, self.at = me, term, core, away, place, at
        self.from_core, self.first, self.second, self.third = buffers
        self.send, self.recv, self.local = sems
        self.count, self.part = term.shape[0], term.shape[-2] // 4
        self.stage = -1

    def rows(self, where):
        return pl.ds(pl.multiple_of(where * self.part, self.part), self.part)

    def axes(self, color):
        main, other = ("y", "z") if color == 0 else ("z", "y")
        return main, other, self.rows(getattr(self.me, main))

    def copies(self, stage):
        me, term, core, made = self.me, self.term, self.core, []

        def copy(src, dst, color, k, device):
            at = (*self.at, stage, color, k)
            made.append(pltpu.make_async_remote_copy(src_ref=src, dst_ref=dst, send_sem=self.send.at[at], recv_sem=self.recv.at[at], device_id=device, device_id_type=MESH))

        if stage == 0:
            for n, (src, dst) in enumerate(self.away):
                copy(src, dst, n, 0, me.partner())
            return made
        for color in range(2):
            main, other, mine = self.axes(color)
            for k in range(3):
                there, device = me.along({2: "x", 3: other}.get(stage, main), k + 1)
                if stage == 1:
                    copy(term.at[:, color, :, core, self.rows(there)], self.first.at[:, color, k], color, k, device)
                elif stage == 2:
                    copy(term.at[:, color, there, core, mine], self.second.at[:, color, k], color, k, device)
                elif stage == 3:
                    copy(term.at[:, color, me.x, core, mine], self.third.at[:, color, getattr(me, other)], color, k, device)
                else:
                    for n, (src, dst) in enumerate(self.outward(color)):
                        copy(src, dst, color, 3 * n + k, device)
        return made

    def outward(self, color):
        rows = self.axes(color)[-1]
        return [(self.term.at[n, color, self.me.x, self.core, rows], self.place(n, color, rows)) for n in range(self.count)]

    def kept(self):
        return [pltpu.make_async_copy(src, dst, self.local.at[(*self.at, color, n)]) for color in range(2) for n, (src, dst) in enumerate(self.outward(color))]

    def advance(self):
        assert self.stage < STAGES
        if self.stage >= 0:
            self.finish(self.stage)
        self.stage += 1
        if self.stage < STAGES:
            self.start(self.stage)

    def start(self, stage):
        me = self.me
        if stage == 3:
            for color in range(2):
                _, other, rows = self.axes(color)
                self.third[:, color, getattr(me, other)] = self.term[:, color, me.x, self.core, rows]
        for one in self.copies(stage):
            one.start()
        if stage == 4:
            for one in self.kept():
                one.start()

    def finish(self, stage):
        me, term, core = self.me, self.term, self.core
        for one in self.copies(stage):
            one.wait()
        if stage == 4:
            for one in self.kept():
                one.wait()
            return

        @pl.loop(0, self.count)
        def _(n):
            for color in range(2):
                mine = self.axes(color)[-1]
                if stage <= 1:

                    @pl.loop(0, 4)
                    def _(x, color=color, mine=mine):
                        if stage == 0:

                            @pl.loop(0, 4)
                            def _(quarter):
                                rows = self.rows(quarter)
                                total = term[n, color, x, core, rows].astype(F32) + self.from_core[n, color, x, rows].astype(F32)
                                term[n, color, x, core, rows] = total.astype(BF)

                        else:
                            total = term[n, color, x, core, mine].astype(F32)
                            for k in range(3):
                                total += self.first[n, color, k, x].astype(F32)
                            term[n, color, x, core, mine] = total.astype(BF)

                    continue
                if stage == 2:
                    total = term[n, color, me.x, core, mine].astype(F32)
                    parts = [self.second[n, color, k] for k in range(3)]
                else:
                    total, *parts = [self.third[n, color, k].astype(F32) for k in range(4)]
                for one in parts:
                    total += one.astype(F32)
                term[n, color, me.x, core, mine] = total.astype(BF)


def sum_buffers(tiles, rows, cols, from_core=None):
    part = rows // 4
    return [
        pltpu.VMEM((*(from_core or (tiles,)), 2, 4, rows, cols), BF),
        pltpu.VMEM((tiles, 2, 3, 4, part, cols), BF),
        pltpu.VMEM((tiles, 2, 3, part, cols), BF),
        pltpu.VMEM((tiles, 2, 4, part, cols), BF),
    ]


def sum_sems(*groups):
    dma = pltpu.SemaphoreType.DMA
    return [dma((*groups, STAGES, 2, 6)), dma((*groups, STAGES, 2, 6)), dma((*groups, 2, 2))]


class SummedDown:
    def __init__(self, me, term, own, buffers, sems, load, out):
        half = out.shape[-1] // 2
        cols = [pl.ds(n * half, half) for n in range(2)]
        away = [(term.at[:, 1 - me.c, :, c], buffers[0].at[0, n]) for n, c in enumerate(cols)]
        self.loads = [pltpu.make_async_copy(term.at[:, me.c, :, c], own.at[0, n, :, 0], load.at[n]) for n, c in enumerate(cols)]
        self.sum = Summed(me, own, 0, away, buffers, sems, (), lambda n, color, rows: out.at[rows, cols[color]])

    def advance(self):
        if self.sum.stage < 0:
            for one in self.loads:
                one.start()
        elif self.sum.stage == 0:
            for one in self.loads:
                one.wait()
        self.sum.advance()


def down_scratch():
    rows, half = FF // 8, D // 2
    own = pltpu.VMEM((1, 2, 4, 1, rows, half), BF)
    return [own, *sum_buffers(1, rows, half), *sum_sems(), pltpu.SemaphoreType.DMA((2,))]


def summed_down(me, term, out, scratch):
    return SummedDown(me, term, scratch[0], scratch[1:5], scratch[5:8], scratch[8], out)


def run_schedule(i, schedule, named):
    for at, names in enumerate(schedule):

        @pl.when(i == at)
        def _(names=names):
            for name in names:
                named[name].advance()


GRADS_SCHEDULE = ("", "d", "", "a", "a", "", "d", "b", "ba", "d", "a", "cdb", "ca", "ebcebceceebdace")


def first_layer_kernel(a_ref, dh_ref, wd_ref, by_gate_ref, by_up_ref, down_ref, gd_ref, gg_ref, gu_ref, term, both, *rest):
    i = pl.program_id(0)
    me = Place()
    scratch = len(down_scratch())
    named = {"d": summed_down(me, down_ref, gd_ref, rest[:scratch])}
    from_core, *others = rest[scratch : scratch + 4]
    for number, (first, count) in enumerate(SUM_GROUPS):
        tiles = pl.ds(first, count)
        mine, received = term.at[tiles], from_core.at[number % 2, pl.ds(0, count)]

        def place(n, color, rows, first=first):
            return (gg_ref, gu_ref)[color].at[rows, pl.ds((first + n) * TN, TN)]

        away = [(mine.at[:, :, :, 1 - me.c], received)]
        named["abce"[number]] = Summed(me, mine, me.c, away, [received, *(one.at[tiles] for one in others)], rest[scratch + 4 :], (number,), place)

    @pl.when(i == 0)
    def _():
        all_greet(me)
        named["d"].advance()

    half = TN // 2
    for rows in split_rows(TOKENS, 256):
        d = dot(dh_ref[rows, :], wd_ref[...], NT).astype(BF).astype(F32)
        both[rows, :half] = (d * by_gate_ref[rows, :]).astype(BF)
        both[rows, half:] = (d * by_up_ref[rows, :]).astype(BF)
    made = dot(a_ref[...], both[...], TNN).astype(BF)
    cols = pl.ds(pl.multiple_of(lax.rem(i, 2) * half, half), half)
    for n in range(2):
        term[lax.div(i, 2), n, :, :, :, cols] = made[:, n * half : (n + 1) * half].reshape(4, 2, D // 8, half)

    run_schedule(i, GRADS_SCHEDULE, named)


def first_layer_grads(a, dh, wd, by_gate, by_up, down):
    rows_d, rows, tiles, half = FF // 8, D // 8, FF // TN, TN // 2
    anywhere = pl.BlockSpec(memory_space=pl.ANY)
    wide = pl.BlockSpec((TOKENS, D), lambda i: (0, 0), pipeline_mode=pl.Buffered(1))
    tile = pl.BlockSpec((TOKENS, half), lambda i: (0, i))
    gd, gg, gu = pl.pallas_call(
        first_layer_kernel,
        grid=(2 * tiles,),
        in_specs=[wide, wide, pl.BlockSpec((half, D), lambda i: (i, 0)), tile, tile, anywhere],
        out_specs=[anywhere] * 3,
        out_shape=[jax.ShapeDtypeStruct(shape, BF) for shape in ((rows_d, D), (rows, FF), (rows, FF))],
        scratch_shapes=[
            pltpu.VMEM((tiles, 2, 4, 2, rows, TN), BF),
            pltpu.VMEM((TOKENS, TN), BF),
            *down_scratch(),
            *sum_buffers(tiles, rows, TN, (2, 2)),
            *sum_sems(len(SUM_GROUPS)),
        ],
        compiler_params=pltpu.CompilerParams(vmem_limit_bytes=67_043_328, collective_id=0, has_side_effects=True),
        cost_estimate=cost(6 * TOKENS * D * FF, 80 * MIB),
        name="first_layer_grads",
    )(a, dh, wd, by_gate, by_up, down)
    return gg, gu, gd


NORM_SCHEDULE = ("", "", "d", "", "", "", "", "", "", "d", "", "", "", "d", "", "", "d", "", "", "", "d")


def norm_grad_kernel(dg_ref, du_ref, wg_ref, wu_ref, h_ref, dy_ref, hid_ref, down1_ref, dh_ref, down_ref, gd_ref, acc, *rest):
    i, steps, tm = pl.program_id(0), FF // TN, acc.shape[0]
    me = Place()
    named = {"d": summed_down(me, down1_ref, gd_ref, rest)}

    @pl.when(i == 0)
    def _():
        all_greet(me)
        named["d"].advance()

    for part in range(2):
        first = part * steps

        @pl.when(jnp.logical_and(i >= first, i < first + steps))
        def _(part=part, first=first):
            both = dot(dg_ref[...], wg_ref[...], NT) + dot(du_ref[...], wu_ref[...], NT)
            acc[...] = jnp.where(i == first, both, acc[...] + both)

        @pl.when(i == first + steps - 1)
        def _(part=part):
            @pl.loop(0, tm // 128)
            def _(n):
                rows = pl.ds(pl.multiple_of(n * 128, 128), 128)
                da = acc[rows, :].astype(BF).astype(F32)
                wide = h_ref[rows, :].astype(F32)
                scale = lax.rsqrt(jnp.mean(wide * wide, -1, keepdims=True) + 1e-6)
                along = jnp.mean(da * wide, -1, keepdims=True)
                dh = (da * scale - wide * (scale * scale * scale * along)).astype(BF)
                dh_ref[pl.ds(pl.multiple_of(part * tm + n * 128, 128), 128), :] = dy_ref[rows, :] + dh

    @pl.when(i >= 2 * steps)
    def _():
        down_ref[...] = dot(hid_ref[...], dh_ref[...], TNN).astype(BF)

    run_schedule(i, NORM_SCHEDULE, named)


def norm_grad(dg, du, w, h, dy, hid, down1):
    tm, steps = TOKENS // 2, FF // TN

    def k(i):
        return jnp.where(i < 2 * steps, lax.rem(i, steps), steps - 1)

    def m(i):
        return jnp.minimum(lax.div(i, steps), 1)

    def last(i):
        return jnp.maximum(i - 2 * steps, 0)

    anywhere = pl.BlockSpec(memory_space=pl.ANY)
    tile = pl.BlockSpec((tm, TN), lambda i: (m(i), k(i)))
    wide = pl.BlockSpec((tm, D), lambda i: (m(i), 0))
    return pl.pallas_call(
        norm_grad_kernel,
        grid=(3 * steps,),
        in_specs=[
            tile,
            tile,
            pl.BlockSpec((D, TN), lambda i: (0, k(i))),
            pl.BlockSpec((D, TN), lambda i: (0, steps + k(i))),
            wide,
            wide,
            pl.BlockSpec((TOKENS, TN), lambda i: (0, last(i))),
            anywhere,
        ],
        out_specs=[pl.BlockSpec((TOKENS, D), lambda i: (0, 0)), pl.BlockSpec((TN, D), lambda i: (last(i), 0)), anywhere],
        out_shape=[jax.ShapeDtypeStruct(shape, BF) for shape in ((TOKENS, D), (FF, D), (FF // 8, D))],
        scratch_shapes=[pltpu.VMEM((tm, D), F32), *down_scratch()],
        compiler_params=params(collective_id=2, has_side_effects=True),
        cost_estimate=cost(6 * TOKENS * D * FF, 60 * MIB),
        name="norm_grad",
    )(dg, du, w, w, h, dy, hid, down1)


def solution(mesh):
    def step(x, dy, *arrays):
        weights, m, v = (arrays[i : i + 3] for i in (0, 3, 6))
        x, dy = x[0], dy[0]
        place, rows = lax.axis_index("r"), weights[0].shape[1] // 16
        mine = [lax.dynamic_slice(w, (1, place * rows, 0), (1, rows, FF))[0] for w in weights[:2]]
        w1 = lax.all_gather(jnp.concatenate(mine, 1), ("s", "r"), axis=0, tiled=True)

        hid0, by_gate0, by_up0, wd0, wd1, a0 = first_layer_forward(x, *weights)
        h1, a1 = down(hid0, wd0, x)
        hid1, dg1, du1 = last_layer(a1, dy, w1, wd1)

        def scattered(term):
            return lax.psum_scatter(term, "s", scatter_dimension=0, tiled=True)

        terms = [weight_grad(a1, d) for d in (dg1, du1)]
        hid1, *_ = lax.optimization_barrier((hid1, *terms))
        terms = [scattered(one) for one in terms]
        down1 = weight_grad(hid1, dy)
        by_core = (4, 2, FF // 8, D)
        dh1, down0, d1 = norm_grad(dg1, du1, w1, h1, dy, hid0, down1.reshape(by_core))
        *terms, dh1 = lax.optimization_barrier((*terms, dh1))
        g1, u1 = (lax.psum(t, "r") for t in terms)
        g0, u0, d0 = first_layer_grads(a0, dh1, wd0, by_gate0, by_up0, down0.reshape(by_core))
        gradients = [jnp.stack(pair).astype(F32) for pair in ((g0, g1), (u0, u1), (d0, d1))]
        new = [adamw(w.astype(F32), m, v, g) for w, m, v, g in zip(weights, m, v, gradients, strict=True)]
        return tuple(one[which] for which in range(3) for one in new)

    states, cut = P(("rep", "r", "s"), None, None), P(None, "s", None)
    return jax.shard_map(
        step,
        mesh=mesh,
        in_specs=(states, states) + (cut,) * 9,
        out_specs=(P("rep", "s", None),) * 9,
        check_vma=False,
    )
```
